512 devices in a mesh: node: 64 (over z, y), harm: 8 (over x, core).
Axes of the slice: x: 4, y: 8, z: 8, core: 2. Of those that a mesh axis runs over, the one named last changes fastest.
Arguments:
- spectrum: float32 [128, 3, 393216], P('harm', None, 'node'), may hold values from -2 to 2
- source: float32 [128, 3, 393216], P('harm', None, 'node'), may hold values from -4 to 4
- coupling: bfloat16 [3072, 4, 128, 128], P('node'), may hold values from -0.75 to 0.75
- capacitance: float32 [393216], P('node'), may hold values from 0.5 to 4
- saturation: float32 [393216], P('node'), may hold values from 0.1 to 1
- steepness: float32 [393216], P('node'), may hold values from 0.5 to 4
- junction: float32 [393216], P('node'), may hold values from 0.2 to 2
- halo_list: int32 [64, 4, 4], replicated, may hold values from 0 to 47, as said below
- neighbour_slot: int32 [3072, 4], P('node'), may hold values from 0 to 64, as said below
Outputs:
- residual: float32 [128, 3, 393216], P('harm', None, 'node')
The draws below stay inside these ranges and needn't reach their ends.
Inputs may be any that keep to these rules, and one draw needn't show every extreme that they name: `halo_list`: row [m, j] lists 4 distinct blocks of device m, by index among its 48 blocks, needed by the device at index m + o_j along node, o = (-2, -1, 1, 2). `neighbour_slot`: column 0 of block b is b's own index among the 48 blocks of its device d. Other entries v: own block v if v < 48; block halo_list[m, j, s] of device m = d - o_j if v = 48 + j * 4 + s, only where m lies on the mesh; v = 64 is an empty entry. Every such slot of a device whose sender lies on the mesh is named by some entry of the device.
All inputs are finite; a program needn't handle non-finite values.
Results may differ from the reference program's by a relative error of at most 0.0025.
Values may be sent and summed in bfloat16 or wider, within the bound.
A program may use at most 64 MiB of HBM per device.

```python
import math
import jax
import jax.numpy as jnp
from jax import lax

HARMS = 64
SPEC = 128
BLK = 128
NNZ = 4
SLOTS = 4
POINTS = 3
NB_DEV = 48
NBLK = 3072
NODES = 393216
N_NODE = 64


def draw_halo_list(key, part):
    keys = jax.random.split(key, N_NODE * 4)
    chosen = jax.vmap(lambda single: jax.random.permutation(single, NB_DEV)[:SLOTS])(keys)
    return chosen.reshape(N_NODE, 4, SLOTS).astype(jnp.int32)


def draw_neighbour_slot(key, part):
    empty_slot = NB_DEV + 4 * SLOTS
    entries = NB_DEV * (NNZ - 1)

    def per_device(device_key, device):
        first_key, second_key = jax.random.split(device_key)
        halo_slots = NB_DEV + jnp.arange(4 * SLOTS, dtype=jnp.int32)
        others = jax.random.randint(first_key, (entries - 4 * SLOTS,), 0, empty_slot + 1, dtype=jnp.int32)
        mixed = jax.random.permutation(second_key, jnp.concatenate([halo_slots, others]))
        direction = jnp.clip((mixed - NB_DEV) // SLOTS, 0, 3)
        offset = direction - 2 + (direction >= 2).astype(jnp.int32)
        sender = device - offset
        remote = (mixed >= NB_DEV) & (mixed < empty_slot)
        broken = remote & ((sender < 0) | (sender >= N_NODE))
        mixed = jnp.where(broken, empty_slot, mixed)
        own_column = jnp.arange(NB_DEV, dtype=jnp.int32)[:, None]
        return jnp.concatenate([own_column, mixed.reshape(NB_DEV, NNZ - 1)], axis=1)
    device_keys = jax.random.split(key, N_NODE)
    table = jax.vmap(per_device)(device_keys, jnp.arange(N_NODE, dtype=jnp.int32))
    return table.reshape(N_NODE * NB_DEV, NNZ).astype(jnp.int32)


def shard_levels(own_key, dims, cuts, least, top_value):
    factor_of = 1.0
    for dim, blocks in cuts:
        steps = jax.random.uniform(jax.random.fold_in(jax.random.fold_in(own_key, 6), dim), (blocks,), jnp.float32, least / len(cuts), top_value / len(cuts))
        factor_of = factor_of * jnp.repeat(jnp.exp(steps), dims[dim] // blocks).reshape((-1,) + (1,) * (len(dims) - 1 - dim))
    return factor_of


def centred(key, extent, spread, reach, cuts=(), kind=jnp.bfloat16):
    values = jax.random.normal(key, extent, jnp.float32) * spread
    if len(cuts) > 0:
        values = shard_levels(key, extent, cuts, -0.22, 0.18) * values
    return jnp.clip(values, min=-reach, max=reach).astype(kind)


def setup_inputs(seed: int = 0) -> dict:
    key_list = jax.random.split(jax.random.key(seed), 10)
    return {
        "spectrum": centred(key_list[0], (SPEC, POINTS, NODES), 0.15, 2.0, ((0, 8), (2, 64)), jnp.float32),
        "source": centred(key_list[1], (SPEC, POINTS, NODES), 0.3, 4.0, ((0, 8), (2, 64)), jnp.float32),
        "coupling": centred(key_list[2], (NBLK, NNZ, BLK, BLK), (NNZ * BLK // 8) ** -0.5, 0.75, ((0, 64),)),
        "capacitance": jnp.clip(jnp.exp(math.log(4.0) - 2.0794415 * jax.random.uniform(key_list[3], (NODES,), jnp.float32) ** shard_levels(key_list[3], (NODES,), ((0, 64),), -0.2, 0.2)), 0.5, 4.0),
        "saturation": jnp.clip(jnp.exp(math.log(1.0) - 2.3025851 * jax.random.uniform(key_list[4], (NODES,), jnp.float32) ** shard_levels(key_list[4], (NODES,), ((0, 64),), -0.2, 0.2)), 0.1, 1.0),
        "steepness": jnp.clip(jnp.exp(math.log(4.0) - 2.0794415 * jax.random.uniform(key_list[5], (NODES,), jnp.float32) ** shard_levels(key_list[5], (NODES,), ((0, 64),), -0.2, 0.2)), 0.5, 4.0),
        "junction": jnp.clip(jnp.exp(math.log(2.0) - 2.3025851 * jax.random.uniform(key_list[6], (NODES,), jnp.float32) ** shard_levels(key_list[6], (NODES,), ((0, 64),), -0.2, 0.2)), 0.2, 2.0),
        "halo_list": draw_halo_list(jax.random.fold_in(key_list[9], 71), 0),
        "neighbour_slot": draw_neighbour_slot(jax.random.fold_in(key_list[9], 71), 0),
    }


LOG_TWO = 0.6931471805599453

def synthesize(spectra):
    halfway = SPEC // 2
    cosines = spectra[0::2]
    sines = spectra[1::2]
    real_part = jnp.concatenate([cosines[:1] * SPEC, cosines[1:] * halfway, sines[:1] * SPEC], axis=0)
    zero_row = jnp.zeros_like(sines[:1])
    imag_part = jnp.concatenate([zero_row, -sines[1:] * halfway, zero_row], axis=0)
    return jnp.fft.irfft(real_part + 1j * imag_part, n=SPEC, axis=0).astype(jnp.float32)

def analyze(samples):
    halfway = SPEC // 2
    spectra = jnp.fft.rfft(samples, axis=0)
    lowest = spectra[0].real / SPEC
    highest = spectra[halfway].real / SPEC
    cosines = jnp.concatenate([lowest[None], 2.0 * spectra[1:halfway].real / SPEC], axis=0)
    sines = jnp.concatenate([highest[None], -2.0 * spectra[1:halfway].imag / SPEC], axis=0)
    return jnp.stack([cosines, sines], axis=1).reshape(SPEC, samples.shape[1]).astype(jnp.float32)

def derivative(spectra):
    pulsation = jnp.arange(SPEC // 2, dtype=jnp.float32)[:, None] / HARMS
    cosines = spectra[0::2]
    sines = spectra[1::2]
    return jnp.stack([pulsation * sines, -pulsation * cosines], axis=1).reshape(spectra.shape)

def single_level(spectrum, source, coupling, capacitance, saturation, steepness, junction, halo_list, neighbour_slot):
    rounded = spectrum.astype(jnp.bfloat16)
    blocks = rounded.reshape(SPEC, NBLK, BLK).transpose(1, 0, 2)
    offsets = jnp.array([-2, -1, 1, 2], dtype=jnp.int32)
    empty_slot = NB_DEV + 4 * SLOTS

    def per_device(device):
        slots = lax.dynamic_slice_in_dim(neighbour_slot, device * NB_DEV, NB_DEV, 0)
        relative = jnp.clip(slots - NB_DEV, 0, 4 * SLOTS - 1)
        direction = relative // SLOTS
        position = relative % SLOTS
        sender = jnp.clip(device - offsets[direction], 0, N_NODE - 1)
        remote = sender * NB_DEV + halo_list[sender, direction, position]
        global_id = jnp.where(slots < NB_DEV, device * NB_DEV + slots, remote)
        global_id = jnp.where(slots == empty_slot, 0, global_id).astype(jnp.int32)
        keep = (slots != empty_slot).astype(jnp.float32)
        picked = blocks[global_id].astype(jnp.float32) * keep[:, :, None, None]
        matrices = lax.dynamic_slice_in_dim(coupling, device * NB_DEV, NB_DEV, 0).astype(jnp.float32)
        return jnp.einsum('bksj,bkij->bsi', picked, matrices, precision=lax.Precision.HIGHEST)
    coupled = lax.map(per_device, jnp.arange(N_NODE, dtype=jnp.int32))
    coupled = coupled.reshape(NBLK, SPEC, BLK).transpose(1, 0, 2).reshape(SPEC, NODES)
    voltage = synthesize(spectrum)
    current = saturation * (jax.nn.softplus(steepness * voltage) - LOG_TWO)
    charge = junction * voltage / jnp.sqrt(1.0 + voltage * voltage)
    current_spec = analyze(current)
    charge_spec = analyze(charge)
    return coupled + derivative(capacitance * spectrum) + current_spec + derivative(charge_spec) - source

def reference(spectrum, source, coupling, capacitance, saturation, steepness, junction, halo_list, neighbour_slot):
    levels = []
    for level in range(POINTS):
        levels.append(single_level(spectrum[:, level], source[:, level], coupling, capacitance, saturation, steepness, junction, halo_list, neighbour_slot))
    return jnp.stack(levels, axis=1)
```

```python
import functools

import jax
import jax.numpy as jnp
import numpy as np
from jax import lax
from jax.experimental import pallas as pl
from jax.experimental.pallas import tpu as pltpu
from jax.sharding import PartitionSpec as P

OFFSETS = (-2, -1, 1, 2)
LOG2_E = 1.4426950408889634
LN_2 = 0.6931471805599453
MESH = pl.DeviceIdType.MESH
CHUNKS = 3
COUPLING_COPIES = 6


def tables(rows):
    time = np.arange(rows)[:, None]
    row = np.arange(rows)[None, :]
    phase = (row // 2) * time % rows
    angle = 2.0 * np.pi / rows * phase
    synthesis = np.where(row % 2 == 1, np.sin(angle), np.cos(angle))
    synthesis = np.where(row == 1, np.where(time % 2 == 0, 1.0, -1.0), synthesis)
    weights = np.where(np.arange(rows) < 2, 1.0 / rows, 2.0 / rows)
    analysis = synthesis.T * weights[:, None]
    pulsation = (np.arange(rows) // 2)[:, None] / (rows // 2)
    derived = np.empty_like(analysis)
    derived[0::2] = pulsation[0::2] * analysis[1::2]
    derived[1::2] = -pulsation[1::2] * analysis[0::2]
    return synthesis, np.concatenate([analysis, derived], axis=1)


def body(
    n_node,
    n_harm,
    halo_ref,
    slot_ref,
    spectrum_hbm,
    source_hbm,
    coupling_hbm,
    capacitance_ref,
    saturation_ref,
    steepness_ref,
    junction_ref,
    synthesis_ref,
    analysis_ref,
    out_ref,
    spectrum_ref,
    source_ref,
    coupling_ref,
    blocks_ref,
    halo_out_ref,
    halo_in_ref,
    columns_ref,
    back_ref,
    result_ref,
    load_sem,
    halo_send_sem,
    halo_recv_sem,
    there_send_sem,
    there_recv_sem,
    back_send_sem,
    back_recv_sem,
):
    node = lax.axis_index("node")
    harm = lax.axis_index("harm")
    points, spec_rows, _ = spectrum_ref.shape
    block_count, listed, block_size, _ = coupling_ref.shape
    share = block_count // n_harm
    piece = share // CHUNKS
    rows = n_harm * spec_rows
    slots = halo_out_ref.shape[0] // len(OFFSETS)
    neighbours = [lax.rem(node + offset + n_node, n_node) for offset in OFFSETS]

    barrier = pltpu.get_barrier_semaphore()
    for step in range(1, n_harm):
        pl.semaphore_signal(
            barrier, inc=1, device_id=(node, lax.rem(harm + step, n_harm)), device_id_type=MESH
        )
    for neighbour in neighbours:
        pl.semaphore_signal(barrier, inc=1, device_id=(neighbour, harm), device_id_type=MESH)

    load_spectrum = pltpu.make_async_copy(spectrum_hbm, spectrum_ref, load_sem.at[0])
    load_spectrum.start()
    load_source = pltpu.make_async_copy(source_hbm, source_ref, load_sem.at[1])
    per_copy = block_count // COUPLING_COPIES
    load_coupling = [
        pltpu.make_async_copy(
            coupling_hbm.at[pl.ds(i * per_copy, per_copy)],
            coupling_ref.at[pl.ds(i * per_copy, per_copy)],
            load_sem.at[2 + i],
        )
        for i in range(COUPLING_COPIES)
    ]
    for copy in load_coupling:
        copy.start()
    load_source.start()

    load_spectrum.wait()

    def columns_of(b):
        return pl.ds(pl.multiple_of(b * block_size, block_size), block_size)

    def round_block(b, carry):
        blocks_ref[b] = spectrum_ref[:, :, columns_of(b)].astype(jnp.bfloat16)
        return carry

    lax.fori_loop(0, block_count, round_block, 0, unroll=8)
    empty = block_count + len(OFFSETS) * slots
    blocks_ref[empty] = jnp.zeros(blocks_ref.shape[1:], jnp.bfloat16)
    for i in range(len(OFFSETS) * slots):
        halo_out_ref[i] = blocks_ref[halo_ref[i, node]]

    pl.semaphore_wait(barrier, n_harm - 1 + len(OFFSETS))

    halo = []
    for j in range(len(OFFSETS)):
        copy = pltpu.make_async_remote_copy(
            src_ref=halo_out_ref.at[pl.ds(j * slots, slots)],
            dst_ref=halo_in_ref.at[pl.ds(j * slots, slots)],
            send_sem=halo_send_sem.at[j],
            recv_sem=halo_recv_sem.at[j],
            device_id=(neighbours[j], harm),
            device_id_type=MESH,
        )
        copy.start()
        halo.append(copy)
    there = []
    for c in range(CHUNKS):
        for step in range(1, n_harm):
            peer = lax.rem(harm + step, n_harm)
            copy = pltpu.make_async_remote_copy(
                src_ref=blocks_ref.at[pl.ds(peer * share + c * piece, piece)],
                dst_ref=columns_ref.at[harm, pl.ds(c * piece, piece)],
                send_sem=there_send_sem.at[c, step - 1],
                recv_sem=there_recv_sem.at[c, step - 1],
                device_id=(node, peer),
                device_id_type=MESH,
            )
            copy.start()
            there.append(copy)
    columns_ref[harm] = blocks_ref[pl.ds(harm * share, share)]

    for copy in halo:
        copy.wait_recv()
    blocks_ref[pl.ds(block_count, len(OFFSETS) * slots)] = halo_in_ref[...]

    row_index = lax.broadcasted_iota(jnp.int32, (1, 8, block_size), 1)
    even = row_index % 2 == 0
    tiles = spec_rows // 8
    pulsations = []
    for i in range(tiles):
        harmonic = (harm * spec_rows + i * 8 + row_index) // 2
        value = harmonic.astype(jnp.float32) * (2.0 / rows)
        pulsations.append(jnp.where(even, value, -value))
    pulsation = jnp.concatenate(pulsations * points, axis=0)

    def couple(b, carry):
        gathered = jnp.concatenate(
            [
                blocks_ref[slot_ref[k, b]].reshape(points * spec_rows, block_size)
                for k in range(listed)
            ],
            axis=1,
        )
        matrix = jnp.concatenate([coupling_ref[b, k] for k in range(listed)], axis=1)
        coupled = lax.dot_general(
            gathered, matrix, (((1,), (1,)), ((), ())), preferred_element_type=jnp.float32
        )
        columns = columns_of(b)
        stored = capacitance_ref[pl.ds(b, 1)] * spectrum_ref[:, :, columns].reshape(
            points * spec_rows, block_size
        )
        stored = stored.reshape(points * tiles, 8, block_size)
        swapped = jnp.where(even, pltpu.roll(stored, 7, 1), pltpu.roll(stored, 1, 1))
        linear = (pulsation * swapped).reshape(points, spec_rows, block_size)
        out_ref[:, :, columns] = (
            coupled.reshape(points, spec_rows, block_size) + linear - source_ref[:, :, columns]
        )
        return carry

    def couple_part(part):
        count = block_count // COUPLING_COPIES
        load_coupling[part].wait()
        if part == 0:
            load_source.wait()
        lax.fori_loop(part * count, (part + 1) * count, couple, 0, unroll=count)

    back = []

    def nonlinear(c):
        for step in range(1, n_harm):
            there[c * (n_harm - 1) + step - 1].wait_recv()
        for i in range(c * piece, (c + 1) * piece):
            taken = jnp.concatenate(
                [columns_ref[:, i, p].reshape(rows, block_size) for p in range(points)], axis=1
            )
            voltage = jnp.dot(synthesis_ref[...], taken, preferred_element_type=jnp.float32)
            row = pl.ds(harm * share + i, 1)

            def wide(values):
                return jnp.concatenate([values] * points, axis=1)

            steep = wide(steepness_ref[row] * LOG2_E)
            scale = wide(saturation_ref[row] * LN_2)
            junction = wide(junction_ref[row])
            drive = steep * voltage
            current = scale * (
                jnp.maximum(drive, 0.0)
                + jnp.log(1.0 + jnp.exp2(-jnp.abs(drive))) * LOG2_E
                - 1.0
            )
            charge = junction * voltage * lax.rsqrt(1.0 + voltage * voltage)
            both = jnp.concatenate(
                [current.astype(jnp.bfloat16), charge.astype(jnp.bfloat16)], axis=0
            )
            combined = jnp.dot(analysis_ref[...], both, preferred_element_type=jnp.float32)
            combined = combined.astype(jnp.bfloat16)
            for p in range(points):
                back_ref[:, i, p] = combined[:, p * block_size : (p + 1) * block_size].reshape(
                    n_harm, spec_rows, block_size
                )
        for step in range(1, n_harm):
            peer = lax.rem(harm + step, n_harm)
            copy = pltpu.make_async_remote_copy(
                src_ref=back_ref.at[peer, pl.ds(c * piece, piece)],
                dst_ref=result_ref.at[harm, pl.ds(c * piece, piece)],
                send_sem=back_send_sem.at[c, step - 1],
                recv_sem=back_recv_sem.at[c, step - 1],
                device_id=(node, peer),
                device_id_type=MESH,
            )
            copy.start()
            back.append(copy)

    per_chunk = COUPLING_COPIES // CHUNKS
    for c in range(CHUNKS):
        nonlinear(c)
        for part in range(c * per_chunk, (c + 1) * per_chunk):
            couple_part(part)
    result_ref[harm] = back_ref[harm]

    for c in range(CHUNKS):
        for step in range(1, n_harm):
            back[c * (n_harm - 1) + step - 1].wait_recv()
        for q in range(n_harm):
            for i in range(c * piece, (c + 1) * piece):
                b = q * share + i
                span = pl.ds(b * block_size, block_size)
                out_ref[:, :, span] += result_ref[q, i].astype(jnp.float32)

    for copy in halo + there + back:
        copy.wait_send()


def solution(mesh):
    n_node, n_harm = mesh.shape["node"], mesh.shape["harm"]

    def local(
        spectrum,
        source,
        coupling,
        capacitance,
        saturation,
        steepness,
        junction,
        halo_list,
        neighbour_slot,
    ):
        spec_rows, points, node_count = spectrum.shape
        block_count, listed, block_size, _ = coupling.shape
        rows = spec_rows * n_harm
        share = block_count // n_harm
        slots = halo_list.shape[2]
        synthesis, analysis = tables(rows)
        halo_count = len(OFFSETS) * slots
        block = (points, spec_rows, block_size)
        vmem, smem = (pl.BlockSpec(memory_space=s) for s in (pltpu.VMEM, pltpu.SMEM))
        anywhere = pl.BlockSpec(memory_space=pl.ANY)
        dma = pltpu.SemaphoreType.DMA
        result = pl.pallas_call(
            functools.partial(body, n_node, n_harm),
            name="residual",
            out_shape=jax.ShapeDtypeStruct((points, spec_rows, node_count), jnp.float32),
            in_specs=[smem, smem, anywhere, anywhere, anywhere, vmem, vmem, vmem, vmem, vmem, vmem],
            out_specs=vmem,
            scratch_shapes=[
                pltpu.VMEM((points, spec_rows, node_count), jnp.float32),
                pltpu.VMEM((points, spec_rows, node_count), jnp.float32),
                pltpu.VMEM(coupling.shape, jnp.bfloat16),
                pltpu.VMEM((block_count + halo_count + 1, *block), jnp.bfloat16),
                pltpu.VMEM((halo_count, *block), jnp.bfloat16),
                pltpu.VMEM((halo_count, *block), jnp.bfloat16),
                pltpu.VMEM((n_harm, share, *block), jnp.bfloat16),
                pltpu.VMEM((n_harm, share, *block), jnp.bfloat16),
                pltpu.VMEM((n_harm, share, *block), jnp.bfloat16),
                dma((2 + COUPLING_COPIES,)),
                dma((len(OFFSETS),)),
                dma((len(OFFSETS),)),
                dma((CHUNKS, n_harm - 1)),
                dma((CHUNKS, n_harm - 1)),
                dma((CHUNKS, n_harm - 1)),
                dma((CHUNKS, n_harm - 1)),
            ],
            compiler_params=pltpu.CompilerParams(
                collective_id=0, has_side_effects=True, vmem_limit_bytes=40 * 2**20
            ),
        )(
            halo_list.transpose(1, 2, 0).reshape(halo_count, n_node),
            neighbour_slot.T,
            spectrum.transpose(1, 0, 2),
            source.transpose(1, 0, 2),
            coupling,
            capacitance.reshape(block_count, block_size),
            saturation.reshape(block_count, block_size),
            steepness.reshape(block_count, block_size),
            junction.reshape(block_count, block_size),
            jnp.asarray(synthesis, jnp.bfloat16),
            jnp.asarray(analysis, jnp.bfloat16),
        )
        return result.transpose(1, 0, 2)

    return jax.shard_map(
        local,
        mesh=mesh,
        in_specs=(
            P("harm", None, "node"),
            P("harm", None, "node"),
            P("node", None, None, None),
            P("node"),
            P("node"),
            P("node"),
            P("node"),
            P(),
            P("node", None),
        ),
        out_specs=P("harm", None, "node"),
        check_vma=False,
    )
```

```python
import functools

import jax
import jax.numpy as jnp
import numpy as np
from jax import lax
from jax.experimental import pallas as pl
from jax.experimental.pallas import tpu as pltpu
from jax.sharding import PartitionSpec as P

OFFSETS = (-2, -1, 1, 2)
LOG2_E = 1.4426950408889634
LN_2 = 0.6931471805599453
MESH = pl.DeviceIdType.MESH
CHUNKS = 3
COUPLING_COPIES = 6


def tables(rows):
    time = np.arange(rows)[:, None]
    row = np.arange(rows)[None, :]
    phase = (row // 2) * time % rows
    angle = 2.0 * np.pi / rows * phase
    synthesis = np.where(row % 2 == 1, np.sin(angle), np.cos(angle))
    synthesis = np.where(row == 1, np.where(time % 2 == 0, 1.0, -1.0), synthesis)
    weights = np.where(np.arange(rows) < 2, 1.0 / rows, 2.0 / rows)
    analysis = synthesis.T * weights[:, None]
    pulsation = (np.arange(rows) // 2)[:, None] / (rows // 2)
    derived = np.empty_like(analysis)
    derived[0::2] = pulsation[0::2] * analysis[1::2]
    derived[1::2] = -pulsation[1::2] * analysis[0::2]
    return synthesis, np.concatenate([analysis, derived], axis=1)


def body(
    n_node,
    n_harm,
    halo_ref,
    slot_ref,
    spectrum_hbm,
    source_hbm,
    coupling_hbm,
    capacitance_ref,
    saturation_ref,
    steepness_ref,
    junction_ref,
    synthesis_ref,
    analysis_ref,
    out_ref,
    spectrum_ref,
    source_ref,
    coupling_ref,
    blocks_ref,
    halo_out_ref,
    halo_in_ref,
    columns_ref,
    back_ref,
    result_ref,
    load_sem,
    halo_send_sem,
    halo_recv_sem,
    there_send_sem,
    there_recv_sem,
    back_send_sem,
    back_recv_sem,
):
    node = lax.axis_index("node")
    harm = lax.axis_index("harm")
    points, spec_rows, _ = spectrum_ref.shape
    block_count, listed, block_size, _ = coupling_ref.shape
    share = block_count // n_harm
    piece = share // CHUNKS
    rows = n_harm * spec_rows
    slots = halo_out_ref.shape[0] // len(OFFSETS)
    neighbours = [node + offset for offset in OFFSETS]
    on_mesh = [(to >= 0) & (to < n_node) for to in neighbours]
    greeted = sum(is_there.astype(jnp.int32) for is_there in on_mesh)

    barrier = pltpu.get_barrier_semaphore()
    for step in range(1, n_harm):
        pl.semaphore_signal(
            barrier, inc=1, device_id=(node, lax.rem(harm + step, n_harm)), device_id_type=MESH
        )
    for neighbour, is_there in zip(neighbours, on_mesh):

        @pl.when(is_there)
        def _(neighbour=neighbour):
            pl.semaphore_signal(barrier, inc=1, device_id=(neighbour, harm), device_id_type=MESH)


    load_spectrum = pltpu.make_async_copy(spectrum_hbm, spectrum_ref, load_sem.at[0])
    load_spectrum.start()
    load_source = pltpu.make_async_copy(source_hbm, source_ref, load_sem.at[1])
    per_copy = block_count // COUPLING_COPIES
    load_coupling = [
        pltpu.make_async_copy(
            coupling_hbm.at[pl.ds(i * per_copy, per_copy)],
            coupling_ref.at[pl.ds(i * per_copy, per_copy)],
            load_sem.at[2 + i],
        )
        for i in range(COUPLING_COPIES)
    ]
    for copy in load_coupling:
        copy.start()
    load_source.start()

    with jax.named_scope("spectrum_wait"):
        load_spectrum.wait()

    def columns_of(b):
        return pl.ds(pl.multiple_of(b * block_size, block_size), block_size)

    def round_block(b, carry):
        blocks_ref[b] = spectrum_ref[:, :, columns_of(b)].astype(jnp.bfloat16)
        return carry

    with jax.named_scope("round"):
        lax.fori_loop(0, block_count, round_block, 0, unroll=8)
    empty = block_count + len(OFFSETS) * slots
    blocks_ref[empty] = jnp.zeros(blocks_ref.shape[1:], jnp.bfloat16)
    for i in range(len(OFFSETS) * slots):
        halo_out_ref[i] = blocks_ref[halo_ref[i, node]]

    with jax.named_scope("greeting"):
        pl.semaphore_wait(barrier, n_harm - 1 + greeted)

    halo = []
    for j in range(len(OFFSETS)):
        copy = pltpu.make_async_remote_copy(
            src_ref=halo_out_ref.at[pl.ds(j * slots, slots)],
            dst_ref=halo_in_ref.at[pl.ds(j * slots, slots)],
            send_sem=halo_send_sem.at[j],
            recv_sem=halo_recv_sem.at[j],
            device_id=(neighbours[j], harm),
            device_id_type=MESH,
        )
        pl.when(on_mesh[j])(copy.start)
        halo.append(copy)
    there = []
    for c in range(CHUNKS):
        for step in range(1, n_harm):
            peer = lax.rem(harm + step, n_harm)
            copy = pltpu.make_async_remote_copy(
                src_ref=blocks_ref.at[pl.ds(peer * share + c * piece, piece)],
                dst_ref=columns_ref.at[harm, pl.ds(c * piece, piece)],
                send_sem=there_send_sem.at[c, step - 1],
                recv_sem=there_recv_sem.at[c, step - 1],
                device_id=(node, peer),
                device_id_type=MESH,
            )
            copy.start()
            there.append(copy)
    columns_ref[harm] = blocks_ref[pl.ds(harm * share, share)]

    with jax.named_scope("halo_wait"):
        for j, copy in enumerate(halo):
            pl.when(on_mesh[len(OFFSETS) - 1 - j])(copy.wait_recv)
    blocks_ref[pl.ds(block_count, len(OFFSETS) * slots)] = halo_in_ref[...]

    row_index = lax.broadcasted_iota(jnp.int32, (1, 8, block_size), 1)
    even = row_index % 2 == 0
    tiles = spec_rows // 8
    pulsations = []
    for i in range(tiles):
        harmonic = (harm * spec_rows + i * 8 + row_index) // 2
        value = harmonic.astype(jnp.float32) * (2.0 / rows)
        pulsations.append(jnp.where(even, value, -value))
    pulsation = jnp.concatenate(pulsations * points, axis=0)

    def couple(b, carry):
        gathered = jnp.concatenate(
            [
                blocks_ref[slot_ref[k, b]].reshape(points * spec_rows, block_size)
                for k in range(listed)
            ],
            axis=1,
        )
        matrix = jnp.concatenate([coupling_ref[b, k] for k in range(listed)], axis=1)
        coupled = lax.dot_general(
            gathered, matrix, (((1,), (1,)), ((), ())), preferred_element_type=jnp.float32
        )
        columns = columns_of(b)
        stored = capacitance_ref[pl.ds(b, 1)] * spectrum_ref[:, :, columns].reshape(
            points * spec_rows, block_size
        )
        stored = stored.reshape(points * tiles, 8, block_size)
        swapped = jnp.where(even, pltpu.roll(stored, 7, 1), pltpu.roll(stored, 1, 1))
        linear = (pulsation * swapped).reshape(points, spec_rows, block_size)
        out_ref[:, :, columns] = (
            coupled.reshape(points, spec_rows, block_size) + linear - source_ref[:, :, columns]
        )
        return carry

    def couple_part(part):
        count = block_count // COUPLING_COPIES
        load_coupling[part].wait()
        if part == 0:
            load_source.wait()
        with jax.named_scope(f"couple_{part}"):
            lax.fori_loop(part * count, (part + 1) * count, couple, 0, unroll=count)

    back = []

    def nonlinear(c):
        with jax.named_scope(f"there_wait_{c}"):
            for step in range(1, n_harm):
                there[c * (n_harm - 1) + step - 1].wait_recv()
        for i in range(c * piece, (c + 1) * piece):
            taken = jnp.concatenate(
                [columns_ref[:, i, p].reshape(rows, block_size) for p in range(points)], axis=1
            )
            voltage = jnp.dot(synthesis_ref[...], taken, preferred_element_type=jnp.float32)
            row = pl.ds(harm * share + i, 1)

            def wide(values):
                return jnp.concatenate([values] * points, axis=1)

            steep = wide(steepness_ref[row] * LOG2_E)
            scale = wide(saturation_ref[row] * LN_2)
            junction = wide(junction_ref[row])
            drive = steep * voltage
            current = scale * (
                jnp.maximum(drive, 0.0)
                + jnp.log(1.0 + jnp.exp2(-jnp.abs(drive))) * LOG2_E
                - 1.0
            )
            charge = junction * voltage * lax.rsqrt(1.0 + voltage * voltage)
            both = jnp.concatenate(
                [current.astype(jnp.bfloat16), charge.astype(jnp.bfloat16)], axis=0
            )
            combined = jnp.dot(analysis_ref[...], both, preferred_element_type=jnp.float32)
            combined = combined.astype(jnp.bfloat16)
            for p in range(points):
                back_ref[:, i, p] = combined[:, p * block_size : (p + 1) * block_size].reshape(
                    n_harm, spec_rows, block_size
                )
        for step in range(1, n_harm):
            peer = lax.rem(harm + step, n_harm)
            copy = pltpu.make_async_remote_copy(
                src_ref=back_ref.at[peer, pl.ds(c * piece, piece)],
                dst_ref=result_ref.at[harm, pl.ds(c * piece, piece)],
                send_sem=back_send_sem.at[c, step - 1],
                recv_sem=back_recv_sem.at[c, step - 1],
                device_id=(node, peer),
                device_id_type=MESH,
            )
            copy.start()
            back.append(copy)

    per_chunk = COUPLING_COPIES // CHUNKS
    for c in range(CHUNKS):
        nonlinear(c)
        for part in range(c * per_chunk, (c + 1) * per_chunk):
            couple_part(part)
    result_ref[harm] = back_ref[harm]

    for c in range(CHUNKS):
        with jax.named_scope(f"back_wait_{c}"):
            for step in range(1, n_harm):
                back[c * (n_harm - 1) + step - 1].wait_recv()
        for q in range(n_harm):
            for i in range(c * piece, (c + 1) * piece):
                b = q * share + i
                span = pl.ds(b * block_size, block_size)
                out_ref[:, :, span] += result_ref[q, i].astype(jnp.float32)

    for is_there, copy in zip(on_mesh, halo):
        pl.when(is_there)(copy.wait_send)
    for copy in there + back:
        copy.wait_send()


def solution(mesh):
    n_node, n_harm = mesh.shape["node"], mesh.shape["harm"]

    def local(
        spectrum,
        source,
        coupling,
        capacitance,
        saturation,
        steepness,
        junction,
        halo_list,
        neighbour_slot,
    ):
        spec_rows, points, node_count = spectrum.shape
        block_count, listed, block_size, _ = coupling.shape
        rows = spec_rows * n_harm
        share = block_count // n_harm
        slots = halo_list.shape[2]
        synthesis, analysis = tables(rows)
        halo_count = len(OFFSETS) * slots
        block = (points, spec_rows, block_size)
        vmem, smem = (pl.BlockSpec(memory_space=s) for s in (pltpu.VMEM, pltpu.SMEM))
        anywhere = pl.BlockSpec(memory_space=pl.ANY)
        dma = pltpu.SemaphoreType.DMA
        result = pl.pallas_call(
            functools.partial(body, n_node, n_harm),
            name="residual",
            out_shape=jax.ShapeDtypeStruct((points, spec_rows, node_count), jnp.float32),
            in_specs=[smem, smem, anywhere, anywhere, anywhere, vmem, vmem, vmem, vmem, vmem, vmem],
            out_specs=vmem,
            scratch_shapes=[
                pltpu.VMEM((points, spec_rows, node_count), jnp.float32),
                pltpu.VMEM((points, spec_rows, node_count), jnp.float32),
                pltpu.VMEM(coupling.shape, jnp.bfloat16),
                pltpu.VMEM((block_count + halo_count + 1, *block), jnp.bfloat16),
                pltpu.VMEM((halo_count, *block), jnp.bfloat16),
                pltpu.VMEM((halo_count, *block), jnp.bfloat16),
                pltpu.VMEM((n_harm, share, *block), jnp.bfloat16),
                pltpu.VMEM((n_harm, share, *block), jnp.bfloat16),
                pltpu.VMEM((n_harm, share, *block), jnp.bfloat16),
                dma((2 + COUPLING_COPIES,)),
                dma((len(OFFSETS),)),
                dma((len(OFFSETS),)),
                dma((CHUNKS, n_harm - 1)),
                dma((CHUNKS, n_harm - 1)),
                dma((CHUNKS, n_harm - 1)),
                dma((CHUNKS, n_harm - 1)),
            ],
            compiler_params=pltpu.CompilerParams(
                collective_id=0, has_side_effects=True, vmem_limit_bytes=62 * 2**20
            ),
        )(
            halo_list.transpose(1, 2, 0).reshape(halo_count, n_node),
            neighbour_slot.T,
            spectrum.transpose(1, 0, 2),
            source.transpose(1, 0, 2),
            coupling,
            capacitance.reshape(block_count, block_size),
            saturation.reshape(block_count, block_size),
            steepness.reshape(block_count, block_size),
            junction.reshape(block_count, block_size),
            jnp.asarray(synthesis, jnp.bfloat16),
            jnp.asarray(analysis, jnp.bfloat16),
        )
        return result.transpose(1, 0, 2)

    return jax.shard_map(
        local,
        mesh=mesh,
        in_specs=(
            P("harm", None, "node"),
            P("harm", None, "node"),
            P("node", None, None, None),
            P("node"),
            P("node"),
            P("node"),
            P("node"),
            P(),
            P("node", None),
        ),
        out_specs=P("harm", None, "node"),
        check_vma=False,
    )
```

```python
import functools

import jax
import jax.numpy as jnp
import numpy as np
from jax import lax
from jax.experimental import pallas as pl
from jax.experimental.pallas import tpu as pltpu
from jax.sharding import PartitionSpec as P

OFFSETS = (-2, -1, 1, 2)
LOG2_E = 1.4426950408889634
LN_2 = 0.6931471805599453
MESH = pl.DeviceIdType.MESH
CHUNKS = 3
COUPLING_COPIES = 6


def tables(rows):
    time = np.arange(rows)[:, None]
    row = np.arange(rows)[None, :]
    phase = (row // 2) * time % rows
    angle = 2.0 * np.pi / rows * phase
    synthesis = np.where(row % 2 == 1, np.sin(angle), np.cos(angle))
    synthesis = np.where(row == 1, np.where(time % 2 == 0, 1.0, -1.0), synthesis)
    weights = np.where(np.arange(rows) < 2, 1.0 / rows, 2.0 / rows)
    analysis = synthesis.T * weights[:, None]
    pulsation = (np.arange(rows) // 2)[:, None] / (rows // 2)
    derived = np.empty_like(analysis)
    derived[0::2] = pulsation[0::2] * analysis[1::2]
    derived[1::2] = -pulsation[1::2] * analysis[0::2]
    return synthesis, np.concatenate([analysis, derived], axis=1)


def body(
    n_node,
    n_harm,
    halo_hbm,
    slot_hbm,
    spectrum_hbm,
    source_hbm,
    coupling_hbm,
    capacitance_hbm,
    saturation_hbm,
    steepness_hbm,
    junction_hbm,
    synthesis_hbm,
    analysis_hbm,
    out_ref,
    halo_ref,
    slot_ref,
    capacitance_ref,
    saturation_ref,
    steepness_ref,
    junction_ref,
    synthesis_ref,
    analysis_ref,
    spectrum_ref,
    source_ref,
    coupling_ref,
    blocks_ref,
    halo_out_ref,
    halo_in_ref,
    columns_ref,
    back_ref,
    result_ref,
    small_sem,
    load_sem,
    halo_send_sem,
    halo_recv_sem,
    there_send_sem,
    there_recv_sem,
    back_send_sem,
    back_recv_sem,
):
    node = lax.axis_index("node")
    harm = lax.axis_index("harm")
    points, spec_rows, _ = spectrum_ref.shape
    block_count, listed, block_size, _ = coupling_ref.shape
    share = block_count // n_harm
    piece = share // CHUNKS
    rows = n_harm * spec_rows
    slots = halo_out_ref.shape[0] // len(OFFSETS)
    neighbours = [node + offset for offset in OFFSETS]
    on_mesh = [(to >= 0) & (to < n_node) for to in neighbours]
    greeted = sum(is_there.astype(jnp.int32) for is_there in on_mesh)

    load_spectrum = pltpu.make_async_copy(spectrum_hbm, spectrum_ref, load_sem.at[0])
    load_spectrum.start()
    barrier = pltpu.get_barrier_semaphore()
    for step in range(1, n_harm):
        pl.semaphore_signal(
            barrier, inc=1, device_id=(node, lax.rem(harm + step, n_harm)), device_id_type=MESH
        )
    for neighbour, is_there in zip(neighbours, on_mesh):

        @pl.when(is_there)
        def _(neighbour=neighbour):
            pl.semaphore_signal(barrier, inc=1, device_id=(neighbour, harm), device_id_type=MESH)


    whole = [
        (halo_hbm, halo_ref),
        (synthesis_hbm, synthesis_ref),
        (analysis_hbm, analysis_ref),
        (saturation_hbm, saturation_ref),
        (steepness_hbm, steepness_ref),
        (junction_hbm, junction_ref),
        (slot_hbm, slot_ref),
        (capacitance_hbm, capacitance_ref),
        (source_hbm, source_ref),
    ]
    loads = [
        pltpu.make_async_copy(source, target, small_sem.at[i])
        for i, (source, target) in enumerate(whole)
    ]
    per_copy = block_count // COUPLING_COPIES
    load_coupling = [
        pltpu.make_async_copy(
            coupling_hbm.at[pl.ds(i * per_copy, per_copy)],
            coupling_ref.at[pl.ds(i * per_copy, per_copy)],
            load_sem.at[1 + i],
        )
        for i in range(COUPLING_COPIES)
    ]
    load_halo, for_nonlinear, for_linear = loads[0], loads[1:6], loads[6:]
    for copy in loads + load_coupling:
        copy.start()

    with jax.named_scope("spectrum_wait"):
        load_spectrum.wait()

    def columns_of(b):
        return pl.ds(pl.multiple_of(b * block_size, block_size), block_size)

    def round_block(b, carry):
        blocks_ref[b] = spectrum_ref[:, :, columns_of(b)].astype(jnp.bfloat16)
        return carry

    with jax.named_scope("round"):
        lax.fori_loop(0, block_count, round_block, 0, unroll=8)
    empty = block_count + len(OFFSETS) * slots
    blocks_ref[empty] = jnp.zeros(blocks_ref.shape[1:], jnp.bfloat16)
    load_halo.wait()
    for i in range(len(OFFSETS) * slots):
        halo_out_ref[i] = blocks_ref[halo_ref[i, node]]

    with jax.named_scope("greeting"):
        pl.semaphore_wait(barrier, n_harm - 1 + greeted)

    halo = []
    for j in range(len(OFFSETS)):
        copy = pltpu.make_async_remote_copy(
            src_ref=halo_out_ref.at[pl.ds(j * slots, slots)],
            dst_ref=halo_in_ref.at[pl.ds(j * slots, slots)],
            send_sem=halo_send_sem.at[j],
            recv_sem=halo_recv_sem.at[j],
            device_id=(neighbours[j], harm),
            device_id_type=MESH,
        )
        pl.when(on_mesh[j])(copy.start)
        halo.append(copy)
    there = []
    for c in range(CHUNKS):
        for step in range(1, n_harm):
            peer = lax.rem(harm + step, n_harm)
            copy = pltpu.make_async_remote_copy(
                src_ref=blocks_ref.at[pl.ds(peer * share + c * piece, piece)],
                dst_ref=columns_ref.at[harm, pl.ds(c * piece, piece)],
                send_sem=there_send_sem.at[c, step - 1],
                recv_sem=there_recv_sem.at[c, step - 1],
                device_id=(node, peer),
                device_id_type=MESH,
            )
            copy.start()
            there.append(copy)
    columns_ref[harm] = blocks_ref[pl.ds(harm * share, share)]
    for copy in for_nonlinear:
        copy.wait()

    def take_halo():
        with jax.named_scope("halo_wait"):
            for j, copy in enumerate(halo):
                pl.when(on_mesh[len(OFFSETS) - 1 - j])(copy.wait_recv)
        blocks_ref[pl.ds(block_count, len(OFFSETS) * slots)] = halo_in_ref[...]
        for copy in for_linear:
            copy.wait()

    row_index = lax.broadcasted_iota(jnp.int32, (1, 8, block_size), 1)
    even = row_index % 2 == 0
    tiles = spec_rows // 8
    pulsations = []
    for i in range(tiles):
        harmonic = (harm * spec_rows + i * 8 + row_index) // 2
        value = harmonic.astype(jnp.float32) * (2.0 / rows)
        pulsations.append(jnp.where(even, value, -value))
    pulsation = jnp.concatenate(pulsations * points, axis=0)

    def couple(b, carry):
        gathered = jnp.concatenate(
            [
                blocks_ref[slot_ref[k, b]].reshape(points * spec_rows, block_size)
                for k in range(listed)
            ],
            axis=1,
        )
        matrix = jnp.concatenate([coupling_ref[b, k] for k in range(listed)], axis=1)
        coupled = lax.dot_general(
            gathered, matrix, (((1,), (1,)), ((), ())), preferred_element_type=jnp.float32
        )
        columns = columns_of(b)
        stored = capacitance_ref[pl.ds(b, 1)] * spectrum_ref[:, :, columns].reshape(
            points * spec_rows, block_size
        )
        stored = stored.reshape(points * tiles, 8, block_size)
        swapped = jnp.where(even, pltpu.roll(stored, 7, 1), pltpu.roll(stored, 1, 1))
        linear = (pulsation * swapped).reshape(points, spec_rows, block_size)
        out_ref[:, :, columns] = (
            coupled.reshape(points, spec_rows, block_size) + linear - source_ref[:, :, columns]
        )
        return carry

    def couple_part(part):
        count = block_count // COUPLING_COPIES
        load_coupling[part].wait()
        with jax.named_scope(f"couple_{part}"):
            lax.fori_loop(part * count, (part + 1) * count, couple, 0, unroll=count)

    back = []

    def nonlinear(c):
        with jax.named_scope(f"there_wait_{c}"):
            for step in range(1, n_harm):
                there[c * (n_harm - 1) + step - 1].wait_recv()
        for i in range(c * piece, (c + 1) * piece):
            taken = jnp.concatenate(
                [columns_ref[:, i, p].reshape(rows, block_size) for p in range(points)], axis=1
            )
            voltage = jnp.dot(synthesis_ref[...], taken, preferred_element_type=jnp.float32)
            row = pl.ds(harm * share + i, 1)

            def wide(values):
                return jnp.concatenate([values] * points, axis=1)

            steep = wide(steepness_ref[row] * LOG2_E)
            scale = wide(saturation_ref[row] * LN_2)
            junction = wide(junction_ref[row])
            drive = steep * voltage
            current = scale * (
                jnp.maximum(drive, 0.0)
                + jnp.log(1.0 + jnp.exp2(-jnp.abs(drive))) * LOG2_E
                - 1.0
            )
            charge = junction * voltage * lax.rsqrt(1.0 + voltage * voltage)
            both = jnp.concatenate(
                [current.astype(jnp.bfloat16), charge.astype(jnp.bfloat16)], axis=0
            )
            combined = jnp.dot(analysis_ref[...], both, preferred_element_type=jnp.float32)
            combined = combined.astype(jnp.bfloat16)
            for p in range(points):
                back_ref[:, i, p] = combined[:, p * block_size : (p + 1) * block_size].reshape(
                    n_harm, spec_rows, block_size
                )
        for step in range(1, n_harm):
            peer = lax.rem(harm + step, n_harm)
            copy = pltpu.make_async_remote_copy(
                src_ref=back_ref.at[peer, pl.ds(c * piece, piece)],
                dst_ref=result_ref.at[harm, pl.ds(c * piece, piece)],
                send_sem=back_send_sem.at[c, step - 1],
                recv_sem=back_recv_sem.at[c, step - 1],
                device_id=(node, peer),
                device_id_type=MESH,
            )
            copy.start()
            back.append(copy)

    for c in range(CHUNKS):
        nonlinear(c)
        if c == CHUNKS - 2:
            take_halo()
        if c == CHUNKS - 2:
            couple_part(0)
            couple_part(1)
        if c == CHUNKS - 1:
            for part in range(2, COUPLING_COPIES):
                couple_part(part)
    result_ref[harm] = back_ref[harm]

    for c in range(CHUNKS):
        with jax.named_scope(f"back_wait_{c}"):
            for step in range(1, n_harm):
                back[c * (n_harm - 1) + step - 1].wait_recv()
        for q in range(n_harm):
            for i in range(c * piece, (c + 1) * piece):
                b = q * share + i
                span = pl.ds(b * block_size, block_size)
                out_ref[:, :, span] += result_ref[q, i].astype(jnp.float32)

    for is_there, copy in zip(on_mesh, halo):
        pl.when(is_there)(copy.wait_send)
    for copy in there + back:
        copy.wait_send()


def solution(mesh):
    n_node, n_harm = mesh.shape["node"], mesh.shape["harm"]

    def local(
        spectrum,
        source,
        coupling,
        capacitance,
        saturation,
        steepness,
        junction,
        halo_list,
        neighbour_slot,
    ):
        spec_rows, points, node_count = spectrum.shape
        block_count, listed, block_size, _ = coupling.shape
        rows = spec_rows * n_harm
        share = block_count // n_harm
        slots = halo_list.shape[2]
        synthesis, analysis = tables(rows)
        halo_count = len(OFFSETS) * slots
        block = (points, spec_rows, block_size)
        held = functools.partial(pltpu.with_memory_space_constraint, memory_space=pltpu.HBM)
        dma = pltpu.SemaphoreType.DMA
        result = pl.pallas_call(
            functools.partial(body, n_node, n_harm),
            name="residual",
            out_shape=pltpu.VMEM((points, spec_rows, node_count), jnp.float32),
            in_specs=[pl.BlockSpec(memory_space=pltpu.HBM)] * 11,
            out_specs=pl.BlockSpec(memory_space=pltpu.VMEM),
            scratch_shapes=[
                pltpu.SMEM((halo_count, n_node), jnp.int32),
                pltpu.SMEM((listed, block_count), jnp.int32),
                *[pltpu.VMEM((block_count, block_size), jnp.float32)] * 4,
                pltpu.VMEM((rows, rows), jnp.bfloat16),
                pltpu.VMEM((rows, 2 * rows), jnp.bfloat16),
                pltpu.VMEM((points, spec_rows, node_count), jnp.float32),
                pltpu.VMEM((points, spec_rows, node_count), jnp.float32),
                pltpu.VMEM(coupling.shape, jnp.bfloat16),
                pltpu.VMEM((block_count + halo_count + 1, *block), jnp.bfloat16),
                pltpu.VMEM((halo_count, *block), jnp.bfloat16),
                pltpu.VMEM((halo_count, *block), jnp.bfloat16),
                pltpu.VMEM((n_harm, share, *block), jnp.bfloat16),
                pltpu.VMEM((n_harm, share, *block), jnp.bfloat16),
                pltpu.VMEM((n_harm, share, *block), jnp.bfloat16),
                dma((9,)),
                dma((1 + COUPLING_COPIES,)),
                dma((len(OFFSETS),)),
                dma((len(OFFSETS),)),
                dma((CHUNKS, n_harm - 1)),
                dma((CHUNKS, n_harm - 1)),
                dma((CHUNKS, n_harm - 1)),
                dma((CHUNKS, n_harm - 1)),
            ],
            compiler_params=pltpu.CompilerParams(
                collective_id=0, has_side_effects=True, vmem_limit_bytes=40 * 2**20
            ),
        )(
            held(halo_list.transpose(1, 2, 0).reshape(halo_count, n_node)),
            held(neighbour_slot.T),
            held(spectrum.transpose(1, 0, 2)),
            held(source.transpose(1, 0, 2)),
            held(coupling),
            held(capacitance.reshape(block_count, block_size)),
            held(saturation.reshape(block_count, block_size)),
            held(steepness.reshape(block_count, block_size)),
            held(junction.reshape(block_count, block_size)),
            held(jnp.asarray(synthesis, jnp.bfloat16)),
            held(jnp.asarray(analysis, jnp.bfloat16)),
        )
        return result.transpose(1, 0, 2)

    return jax.shard_map(
        local,
        mesh=mesh,
        in_specs=(
            P("harm", None, "node"),
            P("harm", None, "node"),
            P("node", None, None, None),
            P("node"),
            P("node"),
            P("node"),
            P("node"),
            P(),
            P("node", None),
        ),
        out_specs=P("harm", None, "node"),
        check_vma=False,
    )
```

```python
import functools

import jax
import jax.numpy as jnp
import numpy as np
from jax import lax
from jax.experimental import pallas as pl
from jax.experimental.pallas import tpu as pltpu
from jax.sharding import PartitionSpec as P

OFFSETS = (-2, -1, 1, 2)
LOG2_E = 1.4426950408889634
LN_2 = 0.6931471805599453
MESH = pl.DeviceIdType.MESH
CHUNKS = 3
COUPLING_COPIES = 6
Y_SIZE = 8


def tables(rows):
    time = np.arange(rows)[:, None]
    row = np.arange(rows)[None, :]
    phase = (row // 2) * time % rows
    angle = 2.0 * np.pi / rows * phase
    synthesis = np.where(row % 2 == 1, np.sin(angle), np.cos(angle))
    synthesis = np.where(row == 1, np.where(time % 2 == 0, 1.0, -1.0), synthesis)
    weights = np.where(np.arange(rows) < 2, 1.0 / rows, 2.0 / rows)
    analysis = synthesis.T * weights[:, None]
    pulsation = (np.arange(rows) // 2)[:, None] / (rows // 2)
    derived = np.empty_like(analysis)
    derived[0::2] = pulsation[0::2] * analysis[1::2]
    derived[1::2] = -pulsation[1::2] * analysis[0::2]
    return synthesis, np.concatenate([analysis, derived], axis=1)


def body(
    n_node,
    n_harm,
    halo_hbm,
    slot_hbm,
    spectrum_hbm,
    source_hbm,
    coupling_hbm,
    capacitance_hbm,
    saturation_hbm,
    steepness_hbm,
    junction_hbm,
    synthesis_hbm,
    analysis_hbm,
    out_ref,
    halo_ref,
    slot_ref,
    capacitance_ref,
    saturation_ref,
    steepness_ref,
    junction_ref,
    synthesis_ref,
    analysis_ref,
    spectrum_ref,
    source_ref,
    coupling_ref,
    blocks_ref,
    halo_out_ref,
    halo_in_ref,
    columns_ref,
    back_ref,
    result_ref,
    small_sem,
    spectrum_sem,
    coupling_sem,
    halo_send_sem,
    halo_recv_sem,
    there_send_sem,
    there_recv_sem,
    back_send_sem,
    back_recv_sem,
    node_sem,
    late_sem,
):
    node = lax.axis_index("node")
    harm = lax.axis_index("harm")
    points, spec_rows, _ = spectrum_ref.shape
    block_count, listed, block_size, _ = coupling_ref.shape
    span = block_count // CHUNKS
    piece = span // n_harm
    rows = n_harm * spec_rows
    slots = halo_out_ref.shape[0] // len(OFFSETS)
    peers = [lax.rem(harm + step, n_harm) for step in range(1, n_harm)]
    neighbours = [node + offset for offset in OFFSETS]

    last = (node == 0) & (harm == 0)
    with_last = (node == 0) & (harm > 0)

    def nearness(place):
        off = 2 * lax.rem(place, Y_SIZE) - Y_SIZE - 1
        return off * off

    later, earlier = [], []
    for to, offset in zip(neighbours, OFFSETS):
        on_mesh = (to >= 0) & (to < n_node)
        to_near, own_near = nearness(to), nearness(node)
        follows = to_near < own_near
        if offset > 0:
            follows = follows | (to_near == own_near)
        follows = ((to == 0) & (harm == 0)) | (follows & ~last)
        later.append(on_mesh & follows)
        earlier.append(on_mesh & ~follows)

    def count(flags):
        return sum(flag.astype(jnp.int32) for flag in flags)

    barrier = pltpu.get_barrier_semaphore()

    @pl.when(~last)
    def _():
        for peer in peers:
            pl.semaphore_signal(barrier, inc=1, device_id=(node, peer), device_id_type=MESH)

    for neighbour, flag in zip(neighbours, later):

        @pl.when(flag)
        def _(neighbour=neighbour):
            pl.semaphore_signal(barrier, inc=1, device_id=(neighbour, harm), device_id_type=MESH)

    width = span * block_size
    load_spectrum = [
        pltpu.make_async_copy(
            spectrum_hbm.at[:, :, pl.ds(c * width, width)],
            spectrum_ref.at[:, :, pl.ds(c * width, width)],
            spectrum_sem.at[c],
        )
        for c in range(CHUNKS)
    ]
    for copy in load_spectrum:
        copy.start()
    whole = [
        (halo_hbm, halo_ref),
        (synthesis_hbm, synthesis_ref),
        (analysis_hbm, analysis_ref),
        (saturation_hbm, saturation_ref),
        (steepness_hbm, steepness_ref),
        (junction_hbm, junction_ref),
        (slot_hbm, slot_ref),
        (capacitance_hbm, capacitance_ref),
        (source_hbm, source_ref),
    ]
    loads = [
        pltpu.make_async_copy(source, target, small_sem.at[i])
        for i, (source, target) in enumerate(whole)
    ]
    load_halo, for_nonlinear, for_linear = loads[0], loads[1:6], loads[6:]
    load_halo.start()
    for copy in for_nonlinear:
        copy.start()
    per_copy = block_count // COUPLING_COPIES
    load_coupling = [
        pltpu.make_async_copy(
            coupling_hbm.at[pl.ds(i * per_copy, per_copy)],
            coupling_ref.at[pl.ds(i * per_copy, per_copy)],
            coupling_sem.at[i],
        )
        for i in range(COUPLING_COPIES)
    ]

    def columns_of(b):
        return pl.ds(pl.multiple_of(b * block_size, block_size), block_size)

    def round_block(b, carry):
        blocks_ref[b] = spectrum_ref[:, :, columns_of(b)].astype(jnp.bfloat16)
        return carry

    there_chunks = [
        [
            pltpu.make_async_remote_copy(
                src_ref=blocks_ref.at[pl.ds(c * span + peer * piece, piece)],
                dst_ref=columns_ref.at[pl.ds(c * span + harm * piece, piece)],
                send_sem=there_send_sem,
                recv_sem=there_recv_sem.at[c],
                device_id=(node, peer),
                device_id_type=MESH,
            )
            for peer in peers
        ]
        for c in range(CHUNKS)
    ]
    for c in range(CHUNKS):
        with jax.named_scope(f"spectrum_wait_{c}"):
            load_spectrum[c].wait()
        lax.fori_loop(c * span, (c + 1) * span, round_block, 0, unroll=8)
        if c == 0:
            with jax.named_scope("greeting"):
                pl.semaphore_wait(
                    barrier, n_harm - 1 - with_last.astype(jnp.int32) + count(earlier)
                )

            @pl.when(last)
            def _():
                for peer in peers:
                    pl.semaphore_signal(
                        late_sem, inc=1, device_id=(node, peer), device_id_type=MESH
                    )

        for peer, copy in zip(peers, there_chunks[c]):
            pl.when(~(with_last & (peer == 0)))(copy.start)
    for neighbour, flag in zip(neighbours, earlier):

        @pl.when(flag)
        def _(neighbour=neighbour):
            pl.semaphore_signal(node_sem, inc=1, device_id=(neighbour, harm), device_id_type=MESH)

    load_halo.wait()
    for i in range(len(OFFSETS) * slots):
        halo_out_ref[i] = blocks_ref[halo_ref[i, node]]
    empty = block_count + len(OFFSETS) * slots
    blocks_ref[empty] = jnp.zeros(blocks_ref.shape[1:], jnp.bfloat16)
    halo = [
        pltpu.make_async_remote_copy(
            src_ref=halo_out_ref.at[pl.ds(j * slots, slots)],
            dst_ref=halo_in_ref.at[pl.ds(j * slots, slots)],
            send_sem=halo_send_sem.at[j],
            recv_sem=halo_recv_sem.at[j],
            device_id=(neighbour, harm),
            device_id_type=MESH,
        )
        for j, neighbour in enumerate(neighbours)
    ]
    for copy, flag in zip(halo, earlier):
        pl.when(flag)(copy.start)
    for copy in for_linear + load_coupling:
        copy.start()
    for c in range(CHUNKS):
        at = pl.ds(c * span + harm * piece, piece)
        columns_ref[at] = blocks_ref[at]
    for copy in for_nonlinear:
        copy.wait()

    @pl.when(with_last)
    def _():
        with jax.named_scope("last_wait"):
            pl.semaphore_wait(late_sem, 1)
        for chunk in there_chunks:
            for peer, copy in zip(peers, chunk):
                pl.when(peer == 0)(copy.start)

    def bytes_of(buffer, blocks, sem):
        part = buffer.at[pl.ds(0, blocks)]
        return pltpu.make_async_copy(part, part, sem)

    back = []

    def nonlinear(c):
        with jax.named_scope(f"there_wait_{c}"):
            bytes_of(columns_ref, (n_harm - 1) * piece, there_recv_sem.at[c]).wait()
        for i in range(piece):
            taken = jnp.concatenate(
                [
                    jnp.concatenate(
                        [columns_ref[c * span + q * piece + i, p] for q in range(n_harm)], axis=0
                    )
                    for p in range(points)
                ],
                axis=1,
            )
            voltage = jnp.dot(synthesis_ref[...], taken, preferred_element_type=jnp.float32)
            row = pl.ds(c * span + harm * piece + i, 1)

            def wide(values):
                return jnp.concatenate([values] * points, axis=1)

            steep = wide(steepness_ref[row] * LOG2_E)
            scale = wide(saturation_ref[row] * LN_2)
            junction = wide(junction_ref[row])
            drive = steep * voltage
            current = scale * (
                jnp.maximum(drive, 0.0)
                + jnp.log(1.0 + jnp.exp2(-jnp.abs(drive))) * LOG2_E
                - 1.0
            )
            charge = junction * voltage * lax.rsqrt(1.0 + voltage * voltage)
            both = jnp.concatenate(
                [current.astype(jnp.bfloat16), charge.astype(jnp.bfloat16)], axis=0
            )
            combined = jnp.dot(analysis_ref[...], both, preferred_element_type=jnp.float32)
            combined = combined.astype(jnp.bfloat16)
            for q in range(n_harm):
                for p in range(points):
                    back_ref[c * span + q * piece + i, p] = combined[
                        q * spec_rows : (q + 1) * spec_rows,
                        p * block_size : (p + 1) * block_size,
                    ]
        for peer in peers:
            copy = pltpu.make_async_remote_copy(
                src_ref=back_ref.at[pl.ds(c * span + peer * piece, piece)],
                dst_ref=result_ref.at[pl.ds(c * span + harm * piece, piece)],
                send_sem=back_send_sem,
                recv_sem=back_recv_sem.at[c],
                device_id=(node, peer),
                device_id_type=MESH,
            )
            copy.start()
            back.append(copy)

    row_index = lax.broadcasted_iota(jnp.int32, (1, 8, block_size), 1)
    even = row_index % 2 == 0
    tiles = spec_rows // 8
    pulsations = []
    for i in range(tiles):
        harmonic = (harm * spec_rows + i * 8 + row_index) // 2
        value = harmonic.astype(jnp.float32) * (2.0 / rows)
        pulsations.append(jnp.where(even, value, -value))
    pulsation = jnp.concatenate(pulsations * points, axis=0)

    def couple(b, carry):
        gathered = jnp.concatenate(
            [
                blocks_ref[slot_ref[k, b]].reshape(points * spec_rows, block_size)
                for k in range(listed)
            ],
            axis=1,
        )
        matrix = jnp.concatenate([coupling_ref[b, k] for k in range(listed)], axis=1)
        coupled = lax.dot_general(
            gathered, matrix, (((1,), (1,)), ((), ())), preferred_element_type=jnp.float32
        )
        columns = columns_of(b)
        stored = capacitance_ref[pl.ds(b, 1)] * spectrum_ref[:, :, columns].reshape(
            points * spec_rows, block_size
        )
        stored = stored.reshape(points * tiles, 8, block_size)
        swapped = jnp.where(even, pltpu.roll(stored, 7, 1), pltpu.roll(stored, 1, 1))
        linear = (pulsation * swapped).reshape(points, spec_rows, block_size)
        out_ref[:, :, columns] = (
            coupled.reshape(points, spec_rows, block_size) + linear - source_ref[:, :, columns]
        )
        return carry

    nonlinear(0)
    with jax.named_scope("node_wait"):
        awaited = count(later)

        @pl.when(awaited > 0)
        def _():
            pl.semaphore_wait(node_sem, awaited)

    for copy, flag in zip(halo, later):
        pl.when(flag)(copy.start)
    for c in range(1, CHUNKS):
        nonlinear(c)
    for c in range(CHUNKS):
        at = pl.ds(c * span + harm * piece, piece)
        result_ref[at] = back_ref[at]
    with jax.named_scope("halo_wait"):
        for j, copy in enumerate(halo):
            opposite = len(OFFSETS) - 1 - j
            pl.when(later[opposite] | earlier[opposite])(copy.wait_recv)
    blocks_ref[pl.ds(block_count, len(OFFSETS) * slots)] = halo_in_ref[...]
    for copy in for_linear:
        copy.wait()
    for part in range(COUPLING_COPIES):
        load_coupling[part].wait()
        with jax.named_scope(f"couple_{part}"):
            lax.fori_loop(part * per_copy, (part + 1) * per_copy, couple, 0, unroll=per_copy)

    for c in range(CHUNKS):
        with jax.named_scope(f"back_wait_{c}"):
            bytes_of(result_ref, (n_harm - 1) * piece, back_recv_sem.at[c]).wait()
        if c == CHUNKS - 1:
            with jax.named_scope("sent"):
                for copy, up, down in zip(halo, later, earlier):
                    pl.when(up | down)(copy.wait_send)
                sent = CHUNKS * (n_harm - 1) * piece
                bytes_of(blocks_ref, sent, there_send_sem).wait()
                bytes_of(back_ref, sent, back_send_sem).wait()
        with jax.named_scope(f"add_{c}"):
            for b in range(c * span, (c + 1) * span):
                at = pl.ds(b * block_size, block_size)
                out_ref[:, :, at] += result_ref[b].astype(jnp.float32)


def solution(mesh):
    n_node, n_harm = mesh.shape["node"], mesh.shape["harm"]

    def local(
        spectrum,
        source,
        coupling,
        capacitance,
        saturation,
        steepness,
        junction,
        halo_list,
        neighbour_slot,
    ):
        spec_rows, points, node_count = spectrum.shape
        block_count, listed, block_size, _ = coupling.shape
        rows = spec_rows * n_harm
        slots = halo_list.shape[2]
        synthesis, analysis = tables(rows)
        halo_count = len(OFFSETS) * slots
        block = (points, spec_rows, block_size)
        held = functools.partial(pltpu.with_memory_space_constraint, memory_space=pltpu.HBM)
        dma = pltpu.SemaphoreType.DMA
        result = pl.pallas_call(
            functools.partial(body, n_node, n_harm),
            name="residual",
            out_shape=pltpu.VMEM((points, spec_rows, node_count), jnp.float32),
            in_specs=[pl.BlockSpec(memory_space=pltpu.HBM)] * 11,
            out_specs=pl.BlockSpec(memory_space=pltpu.VMEM),
            scratch_shapes=[
                pltpu.SMEM((halo_count, n_node), jnp.int32),
                pltpu.SMEM((listed, block_count), jnp.int32),
                *[pltpu.VMEM((block_count, block_size), jnp.float32)] * 4,
                pltpu.VMEM((rows, rows), jnp.bfloat16),
                pltpu.VMEM((rows, 2 * rows), jnp.bfloat16),
                pltpu.VMEM((points, spec_rows, node_count), jnp.float32),
                pltpu.VMEM((points, spec_rows, node_count), jnp.float32),
                pltpu.VMEM(coupling.shape, jnp.bfloat16),
                pltpu.VMEM((block_count + halo_count + 1, *block), jnp.bfloat16),
                pltpu.VMEM((halo_count, *block), jnp.bfloat16),
                pltpu.VMEM((halo_count, *block), jnp.bfloat16),
                *[pltpu.VMEM((block_count, *block), jnp.bfloat16)] * 3,
                dma((9,)),
                dma((CHUNKS,)),
                dma((COUPLING_COPIES,)),
                dma((len(OFFSETS),)),
                dma((len(OFFSETS),)),
                dma,
                dma((CHUNKS,)),
                dma,
                dma((CHUNKS,)),
                pltpu.SemaphoreType.REGULAR,
                pltpu.SemaphoreType.REGULAR,
            ],
            compiler_params=pltpu.CompilerParams(
                collective_id=0, has_side_effects=True, vmem_limit_bytes=40 * 2**20
            ),
        )(
            held(halo_list.transpose(1, 2, 0).reshape(halo_count, n_node)),
            held(neighbour_slot.T),
            held(spectrum.transpose(1, 0, 2)),
            held(source.transpose(1, 0, 2)),
            held(coupling),
            held(capacitance.reshape(block_count, block_size)),
            held(saturation.reshape(block_count, block_size)),
            held(steepness.reshape(block_count, block_size)),
            held(junction.reshape(block_count, block_size)),
            held(jnp.asarray(synthesis, jnp.bfloat16)),
            held(jnp.asarray(analysis, jnp.bfloat16)),
        )
        return result.transpose(1, 0, 2)

    return jax.shard_map(
        local,
        mesh=mesh,
        in_specs=(
            P("harm", None, "node"),
            P("harm", None, "node"),
            P("node", None, None, None),
            P("node"),
            P("node"),
            P("node"),
            P("node"),
            P(),
            P("node", None),
        ),
        out_specs=P("harm", None, "node"),
        check_vma=False,
    )
```

```python
import functools

import jax
import jax.numpy as jnp
import numpy as np
from jax import lax
from jax.experimental import pallas as pl
from jax.experimental.pallas import tpu as pltpu
from jax.sharding import PartitionSpec as P

OFFSETS = (-2, -1, 1, 2)
LOG2_E = 1.4426950408889634
LN_2 = 0.6931471805599453
MESH = pl.DeviceIdType.MESH
CHUNKS = 3
COUPLING_COPIES = 6
EARLY_PARTS = 3
Y_SIZE = 8


def tables(rows):
    time = np.arange(rows)[:, None]
    row = np.arange(rows)[None, :]
    phase = (row // 2) * time % rows
    angle = 2.0 * np.pi / rows * phase
    synthesis = np.where(row % 2 == 1, np.sin(angle), np.cos(angle))
    synthesis = np.where(row == 1, np.where(time % 2 == 0, 1.0, -1.0), synthesis)
    weights = np.where(np.arange(rows) < 2, 1.0 / rows, 2.0 / rows)
    analysis = synthesis.T * weights[:, None]
    pulsation = (np.arange(rows) // 2)[:, None] / (rows // 2)
    derived = np.empty_like(analysis)
    derived[0::2] = pulsation[0::2] * analysis[1::2]
    derived[1::2] = -pulsation[1::2] * analysis[0::2]
    return synthesis, np.concatenate([analysis, derived], axis=1)


def body(
    n_node,
    n_harm,
    halo_hbm,
    slot_hbm,
    spectrum_hbm,
    source_hbm,
    coupling_hbm,
    capacitance_hbm,
    saturation_hbm,
    steepness_hbm,
    junction_hbm,
    synthesis_hbm,
    analysis_hbm,
    out_ref,
    halo_ref,
    slot_ref,
    capacitance_ref,
    saturation_ref,
    steepness_ref,
    junction_ref,
    synthesis_ref,
    analysis_ref,
    spectrum_ref,
    source_ref,
    coupling_ref,
    blocks_ref,
    halo_out_ref,
    halo_in_ref,
    columns_ref,
    back_ref,
    result_ref,
    small_sem,
    spectrum_sem,
    coupling_sem,
    halo_send_sem,
    halo_recv_sem,
    there_send_sem,
    there_recv_sem,
    back_send_sem,
    back_recv_sem,
    node_sem,
    late_sem,
    proxy_ref,
    proxy_back_ref,
    proxy_sem,
):
    node = lax.axis_index("node")
    harm = lax.axis_index("harm")
    points, spec_rows, _ = spectrum_ref.shape
    block_count, listed, block_size, _ = coupling_ref.shape
    span = block_count // CHUNKS
    piece = span // n_harm
    rows = n_harm * spec_rows
    slots = halo_out_ref.shape[0] // len(OFFSETS)
    chips = n_harm // 2
    turns = [(0, 1)] + [(ahead, core) for core in (0, 1) for ahead in (2, 3, 1)]
    peers = [
        lax.rem(harm // 2 + ahead, chips) * 2 + lax.rem(harm + core, 2) for ahead, core in turns
    ]
    neighbours = [node + offset for offset in OFFSETS]

    last = (node == 0) & (harm == 0)
    with_last = (node == 0) & (harm > 0)
    proxy = (node == 0) & (harm == 1)

    middle = n_node // Y_SIZE // 2

    def upper_follows(lower, distance):
        y, above = lax.rem(lower, Y_SIZE), lower // Y_SIZE + 1
        low_off = 2 * y - Y_SIZE - 1
        high_off = 2 * lax.rem(y + distance, Y_SIZE) - Y_SIZE - 1
        crosses = y + distance >= Y_SIZE
        across = above == middle
        if distance == 2:
            across = across | ((above < middle) & (y == Y_SIZE - 1))
        along = high_off * high_off <= low_off * low_off
        return (crosses & across) | (~crosses & along)

    later, earlier = [], []
    for to, offset in zip(neighbours, OFFSETS):
        on_mesh = (to >= 0) & (to < n_node)
        follows = upper_follows(node, offset) if offset > 0 else ~upper_follows(to, -offset)
        follows = ((to == 0) & (harm == 0)) | (follows & ~last)
        later.append(on_mesh & follows)
        earlier.append(on_mesh & ~follows)

    def count(flags):
        return sum(flag.astype(jnp.int32) for flag in flags)

    width = span * block_size
    load_spectrum = [
        pltpu.make_async_copy(
            spectrum_hbm.at[:, :, pl.ds(c * width, width)],
            spectrum_ref.at[:, :, pl.ds(c * width, width)],
            spectrum_sem.at[c],
        )
        for c in range(CHUNKS)
    ]
    for copy in load_spectrum:
        copy.start()
    barrier = pltpu.get_barrier_semaphore()

    @pl.when(~last)
    def _():
        for peer in peers:
            pl.semaphore_signal(barrier, inc=1, device_id=(node, peer), device_id_type=MESH)

    for neighbour, flag in zip(neighbours, later):

        @pl.when(flag)
        def _(neighbour=neighbour):
            pl.semaphore_signal(barrier, inc=1, device_id=(neighbour, harm), device_id_type=MESH)

    whole = [
        (halo_hbm, halo_ref),
        (synthesis_hbm, synthesis_ref),
        (analysis_hbm, analysis_ref),
        (saturation_hbm, saturation_ref),
        (steepness_hbm, steepness_ref),
        (junction_hbm, junction_ref),
        (slot_hbm, slot_ref),
        (capacitance_hbm, capacitance_ref),
        (source_hbm, source_ref),
    ]
    loads = [
        pltpu.make_async_copy(source, target, small_sem.at[i])
        for i, (source, target) in enumerate(whole)
    ]
    load_halo, for_nonlinear, for_linear = loads[0], loads[1:6], loads[6:]
    load_halo.start()
    for copy in for_nonlinear:
        copy.start()
    per_copy = block_count // COUPLING_COPIES
    load_coupling = [
        pltpu.make_async_copy(
            coupling_hbm.at[pl.ds(i * per_copy, per_copy)],
            coupling_ref.at[pl.ds(i * per_copy, per_copy)],
            coupling_sem.at[i],
        )
        for i in range(COUPLING_COPIES)
    ]

    def columns_of(b):
        return pl.ds(pl.multiple_of(b * block_size, block_size), block_size)

    def round_block(b, carry):
        blocks_ref[b] = spectrum_ref[:, :, columns_of(b)].astype(jnp.bfloat16)
        return carry

    there_chunks = [
        [
            pltpu.make_async_remote_copy(
                src_ref=blocks_ref.at[pl.ds(c * span + peer * piece, piece)],
                dst_ref=columns_ref.at[pl.ds(c * span + harm * piece, piece)],
                send_sem=there_send_sem,
                recv_sem=there_recv_sem.at[c],
                device_id=(node, peer),
                device_id_type=MESH,
            )
            for peer in peers
        ]
        for c in range(CHUNKS)
    ]
    for c in range(CHUNKS):
        with jax.named_scope(f"spectrum_wait_{c}"):
            load_spectrum[c].wait()
        lax.fori_loop(c * span, (c + 1) * span, round_block, 0, unroll=8)
        if c == 0:
            with jax.named_scope("greeting"):
                pl.semaphore_wait(
                    barrier, n_harm - 1 - with_last.astype(jnp.int32) + count(earlier)
                )

            @pl.when(last)
            def _():
                for peer in peers:
                    pl.semaphore_signal(
                        late_sem, inc=1, device_id=(node, peer), device_id_type=MESH
                    )

        for peer, copy in zip(peers, there_chunks[c]):
            pl.when(~(with_last & (peer == 0)))(copy.start)

        @pl.when((node == 0) & ~proxy)
        def _(c=c):
            pltpu.make_async_remote_copy(
                src_ref=blocks_ref.at[pl.ds(c * span, piece)],
                dst_ref=proxy_ref.at[pl.ds(c * span + harm * piece, piece)],
                send_sem=there_send_sem,
                recv_sem=proxy_sem.at[c],
                device_id=(node, 1),
                device_id_type=MESH,
            ).start()

    for neighbour, flag in zip(neighbours, earlier):

        @pl.when(flag)
        def _(neighbour=neighbour):
            pl.semaphore_signal(node_sem, inc=1, device_id=(neighbour, harm), device_id_type=MESH)

    load_halo.wait()
    for i in range(len(OFFSETS) * slots):
        halo_out_ref[i] = blocks_ref[halo_ref[i, node]]
    empty = block_count + len(OFFSETS) * slots
    blocks_ref[empty] = jnp.zeros(blocks_ref.shape[1:], jnp.bfloat16)
    halo = [
        pltpu.make_async_remote_copy(
            src_ref=halo_out_ref.at[pl.ds(j * slots, slots)],
            dst_ref=halo_in_ref.at[pl.ds(j * slots, slots)],
            send_sem=halo_send_sem.at[j],
            recv_sem=halo_recv_sem.at[j],
            device_id=(neighbour, harm),
            device_id_type=MESH,
        )
        for j, neighbour in enumerate(neighbours)
    ]
    for copy, flag in zip(halo, earlier):
        pl.when(flag)(copy.start)
    for copy in for_linear + load_coupling:
        copy.start()
    for c in range(CHUNKS):
        at = pl.ds(c * span + harm * piece, piece)
        columns_ref[at] = blocks_ref[at]

    @pl.when(proxy)
    def _():
        for c in range(CHUNKS):
            proxy_ref[pl.ds(c * span + piece, piece)] = blocks_ref[pl.ds(c * span, piece)]

    for copy in for_nonlinear:
        copy.wait()

    def bytes_of(buffer, blocks, sem):
        part = buffer.at[pl.ds(0, blocks)]
        return pltpu.make_async_copy(part, part, sem)

    def evaluate(row, read, write):
        taken = jnp.concatenate(
            [jnp.concatenate([read(q, p) for q in range(n_harm)], axis=0) for p in range(points)],
            axis=1,
        )
        voltage = jnp.dot(synthesis_ref[...], taken, preferred_element_type=jnp.float32)

        def wide(values):
            return jnp.concatenate([values] * points, axis=1)

        steep = wide(steepness_ref[row] * LOG2_E)
        scale = wide(saturation_ref[row] * LN_2)
        junction = wide(junction_ref[row])
        drive = steep * voltage
        current = scale * (
            jnp.maximum(drive, 0.0) + jnp.log(1.0 + jnp.exp2(-jnp.abs(drive))) * LOG2_E - 1.0
        )
        charge = junction * voltage * lax.rsqrt(1.0 + voltage * voltage)
        both = jnp.concatenate([current.astype(jnp.bfloat16), charge.astype(jnp.bfloat16)], axis=0)
        combined = jnp.dot(analysis_ref[...], both, preferred_element_type=jnp.float32)
        combined = combined.astype(jnp.bfloat16)
        for q in range(n_harm):
            for p in range(points):
                write(
                    q,
                    p,
                    combined[
                        q * spec_rows : (q + 1) * spec_rows,
                        p * block_size : (p + 1) * block_size,
                    ],
                )

    def evaluate_chunk(c, owner, taken_ref, given_ref, send_sem):
        for i in range(piece):

            def read(q, p):
                return taken_ref[c * span + q * piece + i, p]

            def write(q, p, values):
                given_ref[c * span + q * piece + i, p] = values

            evaluate(pl.ds(c * span + owner * piece + i, 1), read, write)
        for peer in peers:
            pltpu.make_async_remote_copy(
                src_ref=given_ref.at[pl.ds(c * span + peer * piece, piece)],
                dst_ref=result_ref.at[pl.ds(c * span + owner * piece, piece)],
                send_sem=send_sem,
                recv_sem=back_recv_sem.at[c],
                device_id=(node, peer),
                device_id_type=MESH,
            ).start()
        result_ref[pl.ds(c * span + owner * piece, piece)] = given_ref[
            pl.ds(c * span + harm * piece, piece)
        ]

    whole_share = (n_harm - 1) * piece

    def nonlinear(c):
        with jax.named_scope(f"there_wait_{c}"):
            bytes_of(columns_ref, whole_share, there_recv_sem.at[c]).wait()
        if c == 0:

            @pl.when(with_last)
            def _():
                with jax.named_scope("last_wait"):
                    pl.semaphore_wait(late_sem, 1)

        evaluate_chunk(c, harm, columns_ref, back_ref, back_send_sem)

        @pl.when(proxy)
        def _():
            with jax.named_scope(f"proxy_wait_{c}"):
                bytes_of(proxy_ref, whole_share, proxy_sem.at[c]).wait()
            evaluate_chunk(c, 0, proxy_ref, proxy_back_ref, proxy_sem.at[CHUNKS])

    row_index = lax.broadcasted_iota(jnp.int32, (1, 8, block_size), 1)
    even = row_index % 2 == 0
    tiles = spec_rows // 8
    pulsations = []
    for i in range(tiles):
        harmonic = (harm * spec_rows + i * 8 + row_index) // 2
        value = harmonic.astype(jnp.float32) * (2.0 / rows)
        pulsations.append(jnp.where(even, value, -value))
    pulsation = jnp.concatenate(pulsations * points, axis=0)

    def couple(b, carry):
        gathered = jnp.concatenate(
            [
                blocks_ref[slot_ref[k, b]].reshape(points * spec_rows, block_size)
                for k in range(listed)
            ],
            axis=1,
        )
        matrix = jnp.concatenate([coupling_ref[b, k] for k in range(listed)], axis=1)
        coupled = lax.dot_general(
            gathered, matrix, (((1,), (1,)), ((), ())), preferred_element_type=jnp.float32
        )
        columns = columns_of(b)
        stored = capacitance_ref[pl.ds(b, 1)] * spectrum_ref[:, :, columns].reshape(
            points * spec_rows, block_size
        )
        stored = stored.reshape(points * tiles, 8, block_size)
        swapped = jnp.where(even, pltpu.roll(stored, 7, 1), pltpu.roll(stored, 1, 1))
        linear = (pulsation * swapped).reshape(points, spec_rows, block_size)
        out_ref[:, :, columns] = (
            coupled.reshape(points, spec_rows, block_size) + linear - source_ref[:, :, columns]
        )
        return carry

    with jax.named_scope("node_wait"):
        awaited = count(later)

        @pl.when(awaited > 0)
        def _():
            pl.semaphore_wait(node_sem, awaited)

    for copy, flag in zip(halo, later):
        pl.when(flag)(copy.start)

    def take_halo():
        with jax.named_scope("halo_wait"):
            for j, copy in enumerate(halo):
                opposite = len(OFFSETS) - 1 - j
                pl.when(later[opposite] | earlier[opposite])(copy.wait_recv)
        blocks_ref[pl.ds(block_count, len(OFFSETS) * slots)] = halo_in_ref[...]
        for copy in for_linear:
            copy.wait()

    def couple_part(part, carry):
        first = part * per_copy
        pltpu.make_async_copy(
            coupling_hbm.at[pl.ds(first, per_copy)],
            coupling_ref.at[pl.ds(first, per_copy)],
            coupling_sem.at[part],
        ).wait()
        for i in range(per_copy):
            couple(first + i, 0)
        return carry

    early = jnp.where(proxy, EARLY_PARTS, 0)

    @pl.when(proxy)
    def _():
        take_halo()
        with jax.named_scope("couple_early"):
            lax.fori_loop(0, EARLY_PARTS, couple_part, 0)

    @pl.when(~last)
    def _():
        for c in range(CHUNKS):
            nonlinear(c)

    pl.when(~proxy)(take_halo)
    with jax.named_scope("couple"):
        lax.fori_loop(early, COUPLING_COPIES, couple_part, 0)

    def wait_blocks(flag, buffer, blocks, sem):
        pl.when(flag)(lambda: bytes_of(buffer, blocks, sem).wait())

    plain = ~last & ~proxy
    for c in range(CHUNKS):
        with jax.named_scope(f"back_wait_{c}"):
            wait_blocks(plain, result_ref, whole_share, back_recv_sem.at[c])
            wait_blocks(proxy, result_ref, whole_share - piece, back_recv_sem.at[c])
            wait_blocks(last, result_ref, whole_share + piece, back_recv_sem.at[c])
        if c == CHUNKS - 1:
            with jax.named_scope("sent"):
                for copy, up, down in zip(halo, later, earlier):
                    pl.when(up | down)(copy.wait_send)
                wait_blocks(plain, blocks_ref, CHUNKS * whole_share, there_send_sem)
                wait_blocks(proxy, blocks_ref, CHUNKS * (whole_share - piece), there_send_sem)
                wait_blocks(last, blocks_ref, CHUNKS * (whole_share + piece), there_send_sem)
                wait_blocks(~last, back_ref, CHUNKS * whole_share, back_send_sem)
                wait_blocks(proxy, back_ref, CHUNKS * whole_share, proxy_sem.at[CHUNKS])
        with jax.named_scope(f"add_{c}"):
            for b in range(c * span, (c + 1) * span):
                at = pl.ds(b * block_size, block_size)
                out_ref[:, :, at] += result_ref[b].astype(jnp.float32)


def solution(mesh):
    n_node, n_harm = mesh.shape["node"], mesh.shape["harm"]

    def local(
        spectrum,
        source,
        coupling,
        capacitance,
        saturation,
        steepness,
        junction,
        halo_list,
        neighbour_slot,
    ):
        spec_rows, points, node_count = spectrum.shape
        block_count, listed, block_size, _ = coupling.shape
        rows = spec_rows * n_harm
        slots = halo_list.shape[2]
        synthesis, analysis = tables(rows)
        halo_count = len(OFFSETS) * slots
        block = (points, spec_rows, block_size)
        held = functools.partial(pltpu.with_memory_space_constraint, memory_space=pltpu.HBM)
        dma = pltpu.SemaphoreType.DMA
        result = pl.pallas_call(
            functools.partial(body, n_node, n_harm),
            name="residual",
            out_shape=pltpu.VMEM((points, spec_rows, node_count), jnp.float32),
            in_specs=[pl.BlockSpec(memory_space=pltpu.HBM)] * 11,
            out_specs=pl.BlockSpec(memory_space=pltpu.VMEM),
            scratch_shapes=[
                pltpu.SMEM((halo_count, n_node), jnp.int32),
                pltpu.SMEM((listed, block_count), jnp.int32),
                *[pltpu.VMEM((block_count, block_size), jnp.float32)] * 4,
                pltpu.VMEM((rows, rows), jnp.bfloat16),
                pltpu.VMEM((rows, 2 * rows), jnp.bfloat16),
                pltpu.VMEM((points, spec_rows, node_count), jnp.float32),
                pltpu.VMEM((points, spec_rows, node_count), jnp.float32),
                pltpu.VMEM(coupling.shape, jnp.bfloat16),
                pltpu.VMEM((block_count + halo_count + 1, *block), jnp.bfloat16),
                pltpu.VMEM((halo_count, *block), jnp.bfloat16),
                pltpu.VMEM((halo_count, *block), jnp.bfloat16),
                *[pltpu.VMEM((block_count, *block), jnp.bfloat16)] * 3,
                dma((9,)),
                dma((CHUNKS,)),
                dma((COUPLING_COPIES,)),
                dma((len(OFFSETS),)),
                dma((len(OFFSETS),)),
                dma,
                dma((CHUNKS,)),
                dma,
                dma((CHUNKS,)),
                pltpu.SemaphoreType.REGULAR,
                pltpu.SemaphoreType.REGULAR,
                pltpu.VMEM((block_count, *block), jnp.bfloat16),
                pltpu.VMEM((block_count, *block), jnp.bfloat16),
                dma((CHUNKS + 1,)),
            ],
            compiler_params=pltpu.CompilerParams(
                collective_id=0, has_side_effects=True, vmem_limit_bytes=40 * 2**20
            ),
        )(
            held(halo_list.transpose(1, 2, 0).reshape(halo_count, n_node)),
            held(neighbour_slot.T),
            held(spectrum.transpose(1, 0, 2)),
            held(source.transpose(1, 0, 2)),
            held(coupling),
            held(capacitance.reshape(block_count, block_size)),
            held(saturation.reshape(block_count, block_size)),
            held(steepness.reshape(block_count, block_size)),
            held(junction.reshape(block_count, block_size)),
            held(jnp.asarray(synthesis, jnp.bfloat16)),
            held(jnp.asarray(analysis, jnp.bfloat16)),
        )
        return result.transpose(1, 0, 2)

    return jax.shard_map(
        local,
        mesh=mesh,
        in_specs=(
            P("harm", None, "node"),
            P("harm", None, "node"),
            P("node", None, None, None),
            P("node"),
            P("node"),
            P("node"),
            P("node"),
            P(),
            P("node", None),
        ),
        out_specs=P("harm", None, "node"),
        check_vma=False,
    )
```

```python
import functools

import jax
import jax.numpy as jnp
import numpy as np
from jax import lax
from jax.experimental import pallas as pl
from jax.experimental.pallas import tpu as pltpu
from jax.sharding import PartitionSpec as P

OFFSETS = (-2, -1, 1, 2)
LOG2_E = 1.4426950408889634
LN_2 = 0.6931471805599453
MESH = pl.DeviceIdType.MESH
PIECES = (1, 1, 2, 2)
CHUNKS = len(PIECES)
COUPLING_COPIES = 6
EARLY_PARTS = 3
Y_SIZE = 8


def tables(rows):
    time = np.arange(rows)[:, None]
    row = np.arange(rows)[None, :]
    phase = (row // 2) * time % rows
    angle = 2.0 * np.pi / rows * phase
    synthesis = np.where(row % 2 == 1, np.sin(angle), np.cos(angle))
    synthesis = np.where(row == 1, np.where(time % 2 == 0, 1.0, -1.0), synthesis)
    weights = np.where(np.arange(rows) < 2, 1.0 / rows, 2.0 / rows)
    analysis = synthesis.T * weights[:, None]
    pulsation = (np.arange(rows) // 2)[:, None] / (rows // 2)
    derived = np.empty_like(analysis)
    derived[0::2] = pulsation[0::2] * analysis[1::2]
    derived[1::2] = -pulsation[1::2] * analysis[0::2]
    return synthesis, np.concatenate([analysis, derived], axis=1)


def body(
    n_node,
    n_harm,
    halo_hbm,
    slot_hbm,
    spectrum_hbm,
    source_hbm,
    coupling_hbm,
    capacitance_hbm,
    saturation_hbm,
    steepness_hbm,
    junction_hbm,
    synthesis_hbm,
    analysis_hbm,
    out_ref,
    halo_ref,
    slot_ref,
    capacitance_ref,
    saturation_ref,
    steepness_ref,
    junction_ref,
    synthesis_ref,
    analysis_ref,
    spectrum_ref,
    source_ref,
    coupling_ref,
    blocks_ref,
    halo_out_ref,
    halo_in_ref,
    columns_ref,
    back_ref,
    result_ref,
    small_sem,
    spectrum_sem,
    coupling_sem,
    halo_send_sem,
    halo_recv_sem,
    there_send_sem,
    there_recv_sem,
    back_send_sem,
    back_recv_sem,
    node_sem,
    late_sem,
    proxy_ref,
    proxy_back_ref,
    proxy_sem,
):
    node = lax.axis_index("node")
    harm = lax.axis_index("harm")
    points, spec_rows, _ = spectrum_ref.shape
    block_count, listed, block_size, _ = coupling_ref.shape
    share = block_count // n_harm
    starts = [n_harm * sum(PIECES[:c]) for c in range(CHUNKS + 1)]

    def blocks_of(c, owner):
        return pl.ds(starts[c] + owner * PIECES[c], PIECES[c])

    rows = n_harm * spec_rows
    slots = halo_out_ref.shape[0] // len(OFFSETS)
    chips = n_harm // 2
    turns = [(0, 1)] + [(ahead, core) for core in (0, 1) for ahead in (2, 3, 1)]
    peers = [
        lax.rem(harm // 2 + ahead, chips) * 2 + lax.rem(harm + core, 2) for ahead, core in turns
    ]
    neighbours = [node + offset for offset in OFFSETS]

    last = (node == 0) & (harm == 0)
    with_last = (node == 0) & (harm > 0)
    proxy = (node == 0) & (harm == 1)

    middle = n_node // Y_SIZE // 2

    def upper_follows(lower, distance):
        y, above = lax.rem(lower, Y_SIZE), lower // Y_SIZE + 1
        low_off = 2 * y - Y_SIZE - 1
        high_off = 2 * lax.rem(y + distance, Y_SIZE) - Y_SIZE - 1
        crosses = y + distance >= Y_SIZE
        across = above == middle
        if distance == 2:
            across = (above <= middle) & (y == Y_SIZE - 1)
        along = high_off * high_off <= low_off * low_off
        return (crosses & across) | (~crosses & along)

    later, earlier = [], []
    for to, offset in zip(neighbours, OFFSETS):
        on_mesh = (to >= 0) & (to < n_node)
        follows = upper_follows(node, offset) if offset > 0 else ~upper_follows(to, -offset)
        follows = ((to == 0) & (harm == 0)) | (follows & ~last)
        later.append(on_mesh & follows)
        earlier.append(on_mesh & ~follows)

    def count(flags):
        return sum(flag.astype(jnp.int32) for flag in flags)

    load_spectrum = []
    for c in range(CHUNKS):
        at = pl.ds(starts[c] * block_size, (starts[c + 1] - starts[c]) * block_size)
        load_spectrum.append(
            pltpu.make_async_copy(
                spectrum_hbm.at[:, :, at], spectrum_ref.at[:, :, at], spectrum_sem.at[c]
            )
        )
    for copy in load_spectrum:
        copy.start()
    barrier = pltpu.get_barrier_semaphore()

    @pl.when(~last)
    def _():
        for peer in peers:
            pl.semaphore_signal(barrier, inc=1, device_id=(node, peer), device_id_type=MESH)

    for neighbour, flag in zip(neighbours, later):

        @pl.when(flag)
        def _(neighbour=neighbour):
            pl.semaphore_signal(barrier, inc=1, device_id=(neighbour, harm), device_id_type=MESH)

    whole = [
        (halo_hbm, halo_ref),
        (synthesis_hbm, synthesis_ref),
        (analysis_hbm, analysis_ref),
        (saturation_hbm, saturation_ref),
        (steepness_hbm, steepness_ref),
        (junction_hbm, junction_ref),
        (slot_hbm, slot_ref),
        (capacitance_hbm, capacitance_ref),
        (source_hbm, source_ref),
    ]
    loads = [
        pltpu.make_async_copy(source, target, small_sem.at[i])
        for i, (source, target) in enumerate(whole)
    ]
    load_halo, for_nonlinear, for_linear = loads[0], loads[1:6], loads[6:]
    load_halo.start()
    for copy in for_nonlinear:
        copy.start()
    per_copy = block_count // COUPLING_COPIES
    load_coupling = [
        pltpu.make_async_copy(
            coupling_hbm.at[pl.ds(i * per_copy, per_copy)],
            coupling_ref.at[pl.ds(i * per_copy, per_copy)],
            coupling_sem.at[i],
        )
        for i in range(COUPLING_COPIES)
    ]

    def columns_of(b):
        return pl.ds(pl.multiple_of(b * block_size, block_size), block_size)

    def round_block(b, carry):
        blocks_ref[b] = spectrum_ref[:, :, columns_of(b)].astype(jnp.bfloat16)
        return carry

    there_chunks = [
        [
            pltpu.make_async_remote_copy(
                src_ref=blocks_ref.at[blocks_of(c, peer)],
                dst_ref=columns_ref.at[blocks_of(c, harm)],
                send_sem=there_send_sem,
                recv_sem=there_recv_sem.at[c],
                device_id=(node, peer),
                device_id_type=MESH,
            )
            for peer in peers
        ]
        for c in range(CHUNKS)
    ]
    for c in range(CHUNKS):
        with jax.named_scope(f"spectrum_wait_{c}"):
            load_spectrum[c].wait()
        lax.fori_loop(starts[c], starts[c + 1], round_block, 0, unroll=8)
        if c == 0:
            with jax.named_scope("greeting"):
                pl.semaphore_wait(
                    barrier, n_harm - 1 - with_last.astype(jnp.int32) + count(earlier)
                )

        for peer, copy in zip(peers, there_chunks[c]):
            pl.when(~(with_last & (peer == 0)))(copy.start)

        @pl.when((node == 0) & ~proxy)
        def _(c=c):
            pltpu.make_async_remote_copy(
                src_ref=blocks_ref.at[blocks_of(c, 0)],
                dst_ref=proxy_ref.at[blocks_of(c, harm)],
                send_sem=there_send_sem,
                recv_sem=proxy_sem.at[c],
                device_id=(node, 1),
                device_id_type=MESH,
            ).start()

    @pl.when(last)
    def _():
        for peer in peers:
            pl.semaphore_signal(late_sem, inc=1, device_id=(node, peer), device_id_type=MESH)

    for neighbour, flag in zip(neighbours, earlier):

        @pl.when(flag)
        def _(neighbour=neighbour):
            pl.semaphore_signal(node_sem, inc=1, device_id=(neighbour, harm), device_id_type=MESH)

    load_halo.wait()
    for i in range(len(OFFSETS) * slots):
        halo_out_ref[i] = blocks_ref[halo_ref[i, node]]
    empty = block_count + len(OFFSETS) * slots
    blocks_ref[empty] = jnp.zeros(blocks_ref.shape[1:], jnp.bfloat16)
    halo = [
        pltpu.make_async_remote_copy(
            src_ref=halo_out_ref.at[pl.ds(j * slots, slots)],
            dst_ref=halo_in_ref.at[pl.ds(j * slots, slots)],
            send_sem=halo_send_sem.at[j],
            recv_sem=halo_recv_sem.at[j],
            device_id=(neighbour, harm),
            device_id_type=MESH,
        )
        for j, neighbour in enumerate(neighbours)
    ]
    for copy, flag in zip(halo, earlier):
        pl.when(flag)(copy.start)
    for copy in for_linear + load_coupling:
        copy.start()
    for c in range(CHUNKS):
        columns_ref[blocks_of(c, harm)] = blocks_ref[blocks_of(c, harm)]

    @pl.when(proxy)
    def _():
        for c in range(CHUNKS):
            proxy_ref[blocks_of(c, 1)] = blocks_ref[blocks_of(c, 0)]

    for copy in for_nonlinear:
        copy.wait()

    def bytes_of(buffer, blocks, sem):
        part = buffer.at[pl.ds(0, blocks)]
        return pltpu.make_async_copy(part, part, sem)

    def evaluate(row, read, write):
        taken = jnp.concatenate(
            [jnp.concatenate([read(q, p) for q in range(n_harm)], axis=0) for p in range(points)],
            axis=1,
        )
        voltage = jnp.dot(synthesis_ref[...], taken, preferred_element_type=jnp.float32)

        def wide(values):
            return jnp.concatenate([values] * points, axis=1)

        steep = wide(steepness_ref[row] * LOG2_E)
        scale = wide(saturation_ref[row] * LN_2)
        junction = wide(junction_ref[row])
        drive = steep * voltage
        current = scale * (
            jnp.maximum(drive, 0.0) + jnp.log(1.0 + jnp.exp2(-jnp.abs(drive))) * LOG2_E - 1.0
        )
        charge = junction * voltage * lax.rsqrt(1.0 + voltage * voltage)
        both = jnp.concatenate([current.astype(jnp.bfloat16), charge.astype(jnp.bfloat16)], axis=0)
        combined = jnp.dot(analysis_ref[...], both, preferred_element_type=jnp.float32)
        combined = combined.astype(jnp.bfloat16)
        for q in range(n_harm):
            for p in range(points):
                write(
                    q,
                    p,
                    combined[
                        q * spec_rows : (q + 1) * spec_rows,
                        p * block_size : (p + 1) * block_size,
                    ],
                )

    def give(c, owner, given_ref, peer, send_sem):
        return pltpu.make_async_remote_copy(
            src_ref=given_ref.at[blocks_of(c, peer)],
            dst_ref=result_ref.at[blocks_of(c, owner)],
            send_sem=send_sem,
            recv_sem=back_recv_sem.at[c],
            device_id=(node, peer),
            device_id_type=MESH,
        )

    deferring = (node == 0) & (harm > 1)

    def evaluate_chunk(c, owner, taken_ref, given_ref, send_sem):
        for i in range(PIECES[c]):

            def read(q, p):
                return taken_ref[starts[c] + q * PIECES[c] + i, p]

            def write(q, p, values):
                given_ref[starts[c] + q * PIECES[c] + i, p] = values

            evaluate(pl.ds(starts[c] + owner * PIECES[c] + i, 1), read, write)
        order = [(peer, ~(deferring & (peer == 0))) for peer in peers]
        if c == CHUNKS - 1:
            order = [(1, harm != 1), (0, (harm != 0) & ~deferring)] + [
                (peer, peer > 1) for peer in peers
            ]
        for peer, flag in order:
            pl.when(flag)(give(c, owner, given_ref, peer, send_sem).start)
        result_ref[blocks_of(c, owner)] = given_ref[blocks_of(c, harm)]

    def nonlinear(c):
        with jax.named_scope(f"there_wait_{c}"):
            bytes_of(columns_ref, (n_harm - 1) * PIECES[c], there_recv_sem.at[c]).wait()
        if c == 0:

            @pl.when(with_last)
            def _():
                with jax.named_scope("last_wait"):
                    pl.semaphore_wait(late_sem, 1)

        evaluate_chunk(c, harm, columns_ref, back_ref, back_send_sem)

        @pl.when(proxy)
        def _():
            with jax.named_scope(f"proxy_wait_{c}"):
                bytes_of(proxy_ref, (n_harm - 1) * PIECES[c], proxy_sem.at[c]).wait()
            evaluate_chunk(c, 0, proxy_ref, proxy_back_ref, proxy_sem.at[CHUNKS])

    row_index = lax.broadcasted_iota(jnp.int32, (1, 8, block_size), 1)
    even = row_index % 2 == 0
    tiles = spec_rows // 8
    pulsations = []
    for i in range(tiles):
        harmonic = (harm * spec_rows + i * 8 + row_index) // 2
        value = harmonic.astype(jnp.float32) * (2.0 / rows)
        pulsations.append(jnp.where(even, value, -value))
    pulsation = jnp.concatenate(pulsations * points, axis=0)

    def couple(b, carry):
        gathered = jnp.concatenate(
            [
                blocks_ref[slot_ref[k, b]].reshape(points * spec_rows, block_size)
                for k in range(listed)
            ],
            axis=1,
        )
        matrix = jnp.concatenate([coupling_ref[b, k] for k in range(listed)], axis=1)
        coupled = lax.dot_general(
            gathered, matrix, (((1,), (1,)), ((), ())), preferred_element_type=jnp.float32
        )
        columns = columns_of(b)
        stored = capacitance_ref[pl.ds(b, 1)] * spectrum_ref[:, :, columns].reshape(
            points * spec_rows, block_size
        )
        stored = stored.reshape(points * tiles, 8, block_size)
        swapped = jnp.where(even, pltpu.roll(stored, 7, 1), pltpu.roll(stored, 1, 1))
        linear = (pulsation * swapped).reshape(points, spec_rows, block_size)
        out_ref[:, :, columns] = (
            coupled.reshape(points, spec_rows, block_size) + linear - source_ref[:, :, columns]
        )
        return carry

    with jax.named_scope("node_wait"):
        awaited = count(later)

        @pl.when(awaited > 0)
        def _():
            pl.semaphore_wait(node_sem, awaited)

    for copy, flag in zip(halo, later):
        pl.when(flag)(copy.start)

    def take_halo():
        with jax.named_scope("halo_wait"):
            for j, copy in enumerate(halo):
                opposite = len(OFFSETS) - 1 - j
                pl.when(later[opposite] | earlier[opposite])(copy.wait_recv)
        blocks_ref[pl.ds(block_count, len(OFFSETS) * slots)] = halo_in_ref[...]
        for copy in for_linear:
            copy.wait()

    def couple_part(part, carry):
        first = part * per_copy
        pltpu.make_async_copy(
            coupling_hbm.at[pl.ds(first, per_copy)],
            coupling_ref.at[pl.ds(first, per_copy)],
            coupling_sem.at[part],
        ).wait()
        for i in range(per_copy):
            couple(first + i, 0)
        return carry

    early = jnp.where(proxy, EARLY_PARTS, 0)

    @pl.when(proxy)
    def _():
        take_halo()
        with jax.named_scope("couple_early"):
            lax.fori_loop(0, EARLY_PARTS, couple_part, 0)

    @pl.when(~last)
    def _():
        for c in range(CHUNKS):
            nonlinear(c)

        @pl.when(deferring)
        def _():
            for c in range(CHUNKS):
                give(c, harm, back_ref, 0, back_send_sem).start()

    pl.when(~proxy)(take_halo)
    with jax.named_scope("couple"):
        lax.fori_loop(early, COUPLING_COPIES, couple_part, 0)

    def wait_blocks(flag, buffer, blocks, sem):
        pl.when(flag)(lambda: bytes_of(buffer, blocks, sem).wait())

    plain = ~last & ~proxy
    for c in range(CHUNKS):
        with jax.named_scope(f"back_wait_{c}"):
            wait_blocks(plain, result_ref, (n_harm - 1) * PIECES[c], back_recv_sem.at[c])
            wait_blocks(proxy, result_ref, (n_harm - 2) * PIECES[c], back_recv_sem.at[c])
            wait_blocks(last, result_ref, n_harm * PIECES[c], back_recv_sem.at[c])
        if c == CHUNKS - 1:
            with jax.named_scope("sent"):
                for copy, up, down in zip(halo, later, earlier):
                    pl.when(up | down)(copy.wait_send)
                wait_blocks(plain, blocks_ref, (n_harm - 1) * share, there_send_sem)
                wait_blocks(proxy, blocks_ref, (n_harm - 2) * share, there_send_sem)
                wait_blocks(last, blocks_ref, n_harm * share, there_send_sem)
                wait_blocks(~last, back_ref, (n_harm - 1) * share, back_send_sem)
                wait_blocks(proxy, back_ref, (n_harm - 1) * share, proxy_sem.at[CHUNKS])
        with jax.named_scope(f"add_{c}"):
            for b in range(starts[c], starts[c + 1]):
                at = pl.ds(b * block_size, block_size)
                out_ref[:, :, at] += result_ref[b].astype(jnp.float32)


def solution(mesh):
    n_node, n_harm = mesh.shape["node"], mesh.shape["harm"]

    def local(
        spectrum,
        source,
        coupling,
        capacitance,
        saturation,
        steepness,
        junction,
        halo_list,
        neighbour_slot,
    ):
        spec_rows, points, node_count = spectrum.shape
        block_count, listed, block_size, _ = coupling.shape
        rows = spec_rows * n_harm
        slots = halo_list.shape[2]
        synthesis, analysis = tables(rows)
        halo_count = len(OFFSETS) * slots
        block = (points, spec_rows, block_size)
        held = functools.partial(pltpu.with_memory_space_constraint, memory_space=pltpu.HBM)
        dma = pltpu.SemaphoreType.DMA
        result = pl.pallas_call(
            functools.partial(body, n_node, n_harm),
            name="residual",
            out_shape=pltpu.VMEM((points, spec_rows, node_count), jnp.float32),
            in_specs=[pl.BlockSpec(memory_space=pltpu.HBM)] * 11,
            out_specs=pl.BlockSpec(memory_space=pltpu.VMEM),
            scratch_shapes=[
                pltpu.SMEM((halo_count, n_node), jnp.int32),
                pltpu.SMEM((listed, block_count), jnp.int32),
                *[pltpu.VMEM((block_count, block_size), jnp.float32)] * 4,
                pltpu.VMEM((rows, rows), jnp.bfloat16),
                pltpu.VMEM((rows, 2 * rows), jnp.bfloat16),
                pltpu.VMEM((points, spec_rows, node_count), jnp.float32),
                pltpu.VMEM((points, spec_rows, node_count), jnp.float32),
                pltpu.VMEM(coupling.shape, jnp.bfloat16),
                pltpu.VMEM((block_count + halo_count + 1, *block), jnp.bfloat16),
                pltpu.VMEM((halo_count, *block), jnp.bfloat16),
                pltpu.VMEM((halo_count, *block), jnp.bfloat16),
                *[pltpu.VMEM((block_count, *block), jnp.bfloat16)] * 3,
                dma((9,)),
                dma((CHUNKS,)),
                dma((COUPLING_COPIES,)),
                dma((len(OFFSETS),)),
                dma((len(OFFSETS),)),
                dma,
                dma((CHUNKS,)),
                dma,
                dma((CHUNKS,)),
                pltpu.SemaphoreType.REGULAR,
                pltpu.SemaphoreType.REGULAR,
                pltpu.VMEM((block_count, *block), jnp.bfloat16),
                pltpu.VMEM((block_count, *block), jnp.bfloat16),
                dma((CHUNKS + 1,)),
            ],
            compiler_params=pltpu.CompilerParams(
                collective_id=0, has_side_effects=True, vmem_limit_bytes=40 * 2**20
            ),
        )(
            held(halo_list.transpose(1, 2, 0).reshape(halo_count, n_node)),
            held(neighbour_slot.T),
            held(spectrum.transpose(1, 0, 2)),
            held(source.transpose(1, 0, 2)),
            held(coupling),
            held(capacitance.reshape(block_count, block_size)),
            held(saturation.reshape(block_count, block_size)),
            held(steepness.reshape(block_count, block_size)),
            held(junction.reshape(block_count, block_size)),
            held(jnp.asarray(synthesis, jnp.bfloat16)),
            held(jnp.asarray(analysis, jnp.bfloat16)),
        )
        return result.transpose(1, 0, 2)

    return jax.shard_map(
        local,
        mesh=mesh,
        in_specs=(
            P("harm", None, "node"),
            P("harm", None, "node"),
            P("node", None, None, None),
            P("node"),
            P("node"),
            P("node"),
            P("node"),
            P(),
            P("node", None),
        ),
        out_specs=P("harm", None, "node"),
        check_vma=False,
    )
```

```python
import functools

import jax
import jax.numpy as jnp
import numpy as np
from jax import lax
from jax.experimental import pallas as pl
from jax.experimental.pallas import tpu as pltpu
from jax.sharding import PartitionSpec as P

OFFSETS = (-2, -1, 1, 2)
LOG2_E = 1.4426950408889634
LN_2 = 0.6931471805599453
MESH = pl.DeviceIdType.MESH
PIECES = (1, 1, 2, 2)
CHUNKS = len(PIECES)
COUPLING_COPIES = 6
EARLY_PARTS = 3
Y_SIZE = 8


def tables(rows):
    time = np.arange(rows)[:, None]
    row = np.arange(rows)[None, :]
    phase = (row // 2) * time % rows
    angle = 2.0 * np.pi / rows * phase
    synthesis = np.where(row % 2 == 1, np.sin(angle), np.cos(angle))
    synthesis = np.where(row == 1, np.where(time % 2 == 0, 1.0, -1.0), synthesis)
    weights = np.where(np.arange(rows) < 2, 1.0 / rows, 2.0 / rows)
    analysis = synthesis.T * weights[:, None]
    pulsation = (np.arange(rows) // 2)[:, None] / (rows // 2)
    derived = np.empty_like(analysis)
    derived[0::2] = pulsation[0::2] * analysis[1::2]
    derived[1::2] = -pulsation[1::2] * analysis[0::2]
    return synthesis, np.concatenate([analysis, derived], axis=1)


def body(
    n_node,
    n_harm,
    halo_hbm,
    slot_hbm,
    spectrum_hbm,
    source_hbm,
    coupling_hbm,
    capacitance_hbm,
    saturation_hbm,
    steepness_hbm,
    junction_hbm,
    synthesis_hbm,
    analysis_hbm,
    out_ref,
    halo_ref,
    slot_ref,
    capacitance_ref,
    saturation_ref,
    steepness_ref,
    junction_ref,
    synthesis_ref,
    analysis_ref,
    spectrum_ref,
    source_ref,
    coupling_ref,
    blocks_ref,
    halo_out_ref,
    halo_in_ref,
    columns_ref,
    back_ref,
    result_ref,
    small_sem,
    spectrum_sem,
    coupling_sem,
    halo_send_sem,
    halo_recv_sem,
    there_send_sem,
    there_recv_sem,
    back_send_sem,
    back_recv_sem,
    node_sem,
    late_sem,
    proxy_ref,
    proxy_back_ref,
    proxy_sem,
):
    node = lax.axis_index("node")
    harm = lax.axis_index("harm")
    points, spec_rows, _ = spectrum_ref.shape
    block_count, listed, block_size, _ = coupling_ref.shape
    share = block_count // n_harm
    starts = [n_harm * sum(PIECES[:c]) for c in range(CHUNKS + 1)]

    def blocks_of(c, owner):
        return pl.ds(starts[c] + owner * PIECES[c], PIECES[c])

    rows = n_harm * spec_rows
    slots = halo_out_ref.shape[0] // len(OFFSETS)
    chips = n_harm // 2
    turns = [(0, 1)] + [(ahead, core) for core in (0, 1) for ahead in (2, 3, 1)]
    peers = [
        lax.rem(harm // 2 + ahead, chips) * 2 + lax.rem(harm + core, 2) for ahead, core in turns
    ]
    neighbours = [node + offset for offset in OFFSETS]

    last = (node == 0) & (harm == 0)
    with_last = (node == 0) & (harm > 0)
    proxy = (node == 0) & (harm == 1)

    middle = n_node // Y_SIZE // 2
    halves = lax.rem(harm // 2, 2) == 1

    def upper_follows(lower, distance):
        y, above = lax.rem(lower, Y_SIZE), lower // Y_SIZE + 1
        low_off = 2 * y - Y_SIZE - 1
        high_off = 2 * lax.rem(y + distance, Y_SIZE) - Y_SIZE - 1
        crosses = y + distance >= Y_SIZE
        across = (above == middle) & halves
        if distance == 2:
            far = y == Y_SIZE - 1
            across = across | ((above < middle) & far & halves) | ((above == middle) & far)
        along = high_off * high_off <= low_off * low_off
        return (crosses & across) | (~crosses & along)

    later, earlier = [], []
    for to, offset in zip(neighbours, OFFSETS):
        on_mesh = (to >= 0) & (to < n_node)
        follows = upper_follows(node, offset) if offset > 0 else ~upper_follows(to, -offset)
        follows = ((to == 0) & (harm == 0)) | (follows & ~last)
        later.append(on_mesh & follows)
        earlier.append(on_mesh & ~follows)

    def count(flags):
        return sum(flag.astype(jnp.int32) for flag in flags)

    load_spectrum = []
    for c in range(CHUNKS):
        at = pl.ds(starts[c] * block_size, (starts[c + 1] - starts[c]) * block_size)
        load_spectrum.append(
            pltpu.make_async_copy(
                spectrum_hbm.at[:, :, at], spectrum_ref.at[:, :, at], spectrum_sem.at[c]
            )
        )
    for copy in load_spectrum:
        copy.start()
    barrier = pltpu.get_barrier_semaphore()

    @pl.when(~last)
    def _():
        for peer in peers:
            pl.semaphore_signal(barrier, inc=1, device_id=(node, peer), device_id_type=MESH)

    for neighbour, flag in zip(neighbours, later):

        @pl.when(flag)
        def _(neighbour=neighbour):
            pl.semaphore_signal(barrier, inc=1, device_id=(neighbour, harm), device_id_type=MESH)

    whole = [
        (halo_hbm, halo_ref),
        (synthesis_hbm, synthesis_ref),
        (analysis_hbm, analysis_ref),
        (saturation_hbm, saturation_ref),
        (steepness_hbm, steepness_ref),
        (junction_hbm, junction_ref),
        (slot_hbm, slot_ref),
        (capacitance_hbm, capacitance_ref),
        (source_hbm, source_ref),
    ]
    loads = [
        pltpu.make_async_copy(source, target, small_sem.at[i])
        for i, (source, target) in enumerate(whole)
    ]
    load_halo, for_nonlinear, for_linear = loads[0], loads[1:6], loads[6:]
    load_halo.start()
    for copy in for_nonlinear:
        copy.start()
    per_copy = block_count // COUPLING_COPIES
    load_coupling = [
        pltpu.make_async_copy(
            coupling_hbm.at[pl.ds(i * per_copy, per_copy)],
            coupling_ref.at[pl.ds(i * per_copy, per_copy)],
            coupling_sem.at[i],
        )
        for i in range(COUPLING_COPIES)
    ]

    def columns_of(b):
        return pl.ds(pl.multiple_of(b * block_size, block_size), block_size)

    def round_block(b, carry):
        blocks_ref[b] = spectrum_ref[:, :, columns_of(b)].astype(jnp.bfloat16)
        return carry

    there_chunks = [
        [
            pltpu.make_async_remote_copy(
                src_ref=blocks_ref.at[blocks_of(c, peer)],
                dst_ref=columns_ref.at[blocks_of(c, harm)],
                send_sem=there_send_sem,
                recv_sem=there_recv_sem.at[c],
                device_id=(node, peer),
                device_id_type=MESH,
            )
            for peer in peers
        ]
        for c in range(CHUNKS)
    ]
    for c in range(CHUNKS):
        with jax.named_scope(f"spectrum_wait_{c}"):
            load_spectrum[c].wait()
        lax.fori_loop(starts[c], starts[c + 1], round_block, 0, unroll=8)
        if c == 0:
            with jax.named_scope("greeting"):
                pl.semaphore_wait(
                    barrier, n_harm - 1 - with_last.astype(jnp.int32) + count(earlier)
                )

        for peer, copy in zip(peers, there_chunks[c]):
            pl.when(~(with_last & (peer == 0)))(copy.start)

        @pl.when((node == 0) & ~proxy)
        def _(c=c):
            pltpu.make_async_remote_copy(
                src_ref=blocks_ref.at[blocks_of(c, 0)],
                dst_ref=proxy_ref.at[blocks_of(c, harm)],
                send_sem=there_send_sem,
                recv_sem=proxy_sem.at[c],
                device_id=(node, 1),
                device_id_type=MESH,
            ).start()

    @pl.when(last)
    def _():
        for peer in peers:
            pl.semaphore_signal(late_sem, inc=1, device_id=(node, peer), device_id_type=MESH)

    for neighbour, flag in zip(neighbours, earlier):

        @pl.when(flag)
        def _(neighbour=neighbour):
            pl.semaphore_signal(node_sem, inc=1, device_id=(neighbour, harm), device_id_type=MESH)

    load_halo.wait()
    for i in range(len(OFFSETS) * slots):
        halo_out_ref[i] = blocks_ref[halo_ref[i, node]]
    empty = block_count + len(OFFSETS) * slots
    blocks_ref[empty] = jnp.zeros(blocks_ref.shape[1:], jnp.bfloat16)
    halo = [
        pltpu.make_async_remote_copy(
            src_ref=halo_out_ref.at[pl.ds(j * slots, slots)],
            dst_ref=halo_in_ref.at[pl.ds(j * slots, slots)],
            send_sem=halo_send_sem.at[j],
            recv_sem=halo_recv_sem.at[j],
            device_id=(neighbour, harm),
            device_id_type=MESH,
        )
        for j, neighbour in enumerate(neighbours)
    ]
    for copy, flag in zip(halo, earlier):
        pl.when(flag)(copy.start)
    for copy in for_linear + load_coupling:
        copy.start()
    for c in range(CHUNKS):
        columns_ref[blocks_of(c, harm)] = blocks_ref[blocks_of(c, harm)]

    @pl.when(proxy)
    def _():
        for c in range(CHUNKS):
            proxy_ref[blocks_of(c, 1)] = blocks_ref[blocks_of(c, 0)]

    for copy in for_nonlinear:
        copy.wait()

    def bytes_of(buffer, blocks, sem):
        part = buffer.at[pl.ds(0, blocks)]
        return pltpu.make_async_copy(part, part, sem)

    def evaluate(row, read, write):
        taken = jnp.concatenate(
            [jnp.concatenate([read(q, p) for q in range(n_harm)], axis=0) for p in range(points)],
            axis=1,
        )
        voltage = jnp.dot(synthesis_ref[...], taken, preferred_element_type=jnp.float32)

        def wide(values):
            return jnp.concatenate([values] * points, axis=1)

        steep = wide(steepness_ref[row] * LOG2_E)
        scale = wide(saturation_ref[row] * LN_2)
        junction = wide(junction_ref[row])
        drive = steep * voltage
        current = scale * (
            jnp.maximum(drive, 0.0) + jnp.log(1.0 + jnp.exp2(-jnp.abs(drive))) * LOG2_E - 1.0
        )
        charge = junction * voltage * lax.rsqrt(1.0 + voltage * voltage)
        both = jnp.concatenate([current.astype(jnp.bfloat16), charge.astype(jnp.bfloat16)], axis=0)
        combined = jnp.dot(analysis_ref[...], both, preferred_element_type=jnp.float32)
        combined = combined.astype(jnp.bfloat16)
        for q in range(n_harm):
            for p in range(points):
                write(
                    q,
                    p,
                    combined[
                        q * spec_rows : (q + 1) * spec_rows,
                        p * block_size : (p + 1) * block_size,
                    ],
                )

    def give(c, owner, given_ref, peer, send_sem):
        return pltpu.make_async_remote_copy(
            src_ref=given_ref.at[blocks_of(c, peer)],
            dst_ref=result_ref.at[blocks_of(c, owner)],
            send_sem=send_sem,
            recv_sem=back_recv_sem.at[c],
            device_id=(node, peer),
            device_id_type=MESH,
        )

    deferring = (node == 0) & (harm > 1)

    def evaluate_chunk(c, owner, taken_ref, given_ref, send_sem):
        for i in range(PIECES[c]):

            def read(q, p):
                return taken_ref[starts[c] + q * PIECES[c] + i, p]

            def write(q, p, values):
                given_ref[starts[c] + q * PIECES[c] + i, p] = values

            evaluate(pl.ds(starts[c] + owner * PIECES[c] + i, 1), read, write)
        order = [(peer, ~(deferring & (peer == 0))) for peer in peers]
        if c == CHUNKS - 1:
            order = [(1, harm != 1), (0, (harm != 0) & ~deferring)] + [
                (peer, peer > 1) for peer in peers
            ]
        for peer, flag in order:
            pl.when(flag)(give(c, owner, given_ref, peer, send_sem).start)
        result_ref[blocks_of(c, owner)] = given_ref[blocks_of(c, harm)]

    def nonlinear(c):
        with jax.named_scope(f"there_wait_{c}"):
            bytes_of(columns_ref, (n_harm - 1) * PIECES[c], there_recv_sem.at[c]).wait()
        if c == 0:

            @pl.when(with_last)
            def _():
                with jax.named_scope("last_wait"):
                    pl.semaphore_wait(late_sem, 1)

        evaluate_chunk(c, harm, columns_ref, back_ref, back_send_sem)

        @pl.when(proxy)
        def _():
            with jax.named_scope(f"proxy_wait_{c}"):
                bytes_of(proxy_ref, (n_harm - 1) * PIECES[c], proxy_sem.at[c]).wait()
            evaluate_chunk(c, 0, proxy_ref, proxy_back_ref, proxy_sem.at[CHUNKS])

    row_index = lax.broadcasted_iota(jnp.int32, (1, 8, block_size), 1)
    even = row_index % 2 == 0
    tiles = spec_rows // 8
    pulsations = []
    for i in range(tiles):
        harmonic = (harm * spec_rows + i * 8 + row_index) // 2
        value = harmonic.astype(jnp.float32) * (2.0 / rows)
        pulsations.append(jnp.where(even, value, -value))
    pulsation = jnp.concatenate(pulsations * points, axis=0)

    def couple(b, carry):
        gathered = jnp.concatenate(
            [
                blocks_ref[slot_ref[k, b]].reshape(points * spec_rows, block_size)
                for k in range(listed)
            ],
            axis=1,
        )
        matrix = jnp.concatenate([coupling_ref[b, k] for k in range(listed)], axis=1)
        coupled = lax.dot_general(
            gathered, matrix, (((1,), (1,)), ((), ())), preferred_element_type=jnp.float32
        )
        columns = columns_of(b)
        stored = capacitance_ref[pl.ds(b, 1)] * spectrum_ref[:, :, columns].reshape(
            points * spec_rows, block_size
        )
        stored = stored.reshape(points * tiles, 8, block_size)
        swapped = jnp.where(even, pltpu.roll(stored, 7, 1), pltpu.roll(stored, 1, 1))
        linear = (pulsation * swapped).reshape(points, spec_rows, block_size)
        out_ref[:, :, columns] = (
            coupled.reshape(points, spec_rows, block_size) + linear - source_ref[:, :, columns]
        )
        return carry

    with jax.named_scope("node_wait"):
        awaited = count(later)

        @pl.when(awaited > 0)
        def _():
            pl.semaphore_wait(node_sem, awaited)

    for copy, flag in zip(halo, later):
        pl.when(flag)(copy.start)

    def take_halo():
        with jax.named_scope("halo_wait"):
            for j, copy in enumerate(halo):
                opposite = len(OFFSETS) - 1 - j
                pl.when(later[opposite] | earlier[opposite])(copy.wait_recv)
        blocks_ref[pl.ds(block_count, len(OFFSETS) * slots)] = halo_in_ref[...]
        for copy in for_linear:
            copy.wait()

    def couple_part(part, carry):
        first = part * per_copy
        pltpu.make_async_copy(
            coupling_hbm.at[pl.ds(first, per_copy)],
            coupling_ref.at[pl.ds(first, per_copy)],
            coupling_sem.at[part],
        ).wait()
        for i in range(per_copy):
            couple(first + i, 0)
        return carry

    early = jnp.where(proxy, EARLY_PARTS, 0)

    @pl.when(proxy)
    def _():
        take_halo()
        with jax.named_scope("couple_early"):
            lax.fori_loop(0, EARLY_PARTS, couple_part, 0)

    @pl.when(~last)
    def _():
        for c in range(CHUNKS):
            nonlinear(c)

        @pl.when(deferring)
        def _():
            for c in range(CHUNKS):
                give(c, harm, back_ref, 0, back_send_sem).start()

    pl.when(~proxy)(take_halo)
    with jax.named_scope("couple"):
        lax.fori_loop(early, COUPLING_COPIES, couple_part, 0)

    def wait_blocks(flag, buffer, blocks, sem):
        pl.when(flag)(lambda: bytes_of(buffer, blocks, sem).wait())

    plain = ~last & ~proxy
    for c in range(CHUNKS):
        with jax.named_scope(f"back_wait_{c}"):
            wait_blocks(plain, result_ref, (n_harm - 1) * PIECES[c], back_recv_sem.at[c])
            wait_blocks(proxy, result_ref, (n_harm - 2) * PIECES[c], back_recv_sem.at[c])
            wait_blocks(last, result_ref, n_harm * PIECES[c], back_recv_sem.at[c])
        if c == CHUNKS - 1:
            with jax.named_scope("sent"):
                for copy, up, down in zip(halo, later, earlier):
                    pl.when(up | down)(copy.wait_send)
                wait_blocks(plain, blocks_ref, (n_harm - 1) * share, there_send_sem)
                wait_blocks(proxy, blocks_ref, (n_harm - 2) * share, there_send_sem)
                wait_blocks(last, blocks_ref, n_harm * share, there_send_sem)
                wait_blocks(~last, back_ref, (n_harm - 1) * share, back_send_sem)
                wait_blocks(proxy, back_ref, (n_harm - 1) * share, proxy_sem.at[CHUNKS])
        with jax.named_scope(f"add_{c}"):
            for b in range(starts[c], starts[c + 1]):
                at = pl.ds(b * block_size, block_size)
                out_ref[:, :, at] += result_ref[b].astype(jnp.float32)


def solution(mesh):
    n_node, n_harm = mesh.shape["node"], mesh.shape["harm"]

    def local(
        spectrum,
        source,
        coupling,
        capacitance,
        saturation,
        steepness,
        junction,
        halo_list,
        neighbour_slot,
    ):
        spec_rows, points, node_count = spectrum.shape
        block_count, listed, block_size, _ = coupling.shape
        rows = spec_rows * n_harm
        slots = halo_list.shape[2]
        synthesis, analysis = tables(rows)
        halo_count = len(OFFSETS) * slots
        block = (points, spec_rows, block_size)
        held = functools.partial(pltpu.with_memory_space_constraint, memory_space=pltpu.HBM)
        dma = pltpu.SemaphoreType.DMA
        result = pl.pallas_call(
            functools.partial(body, n_node, n_harm),
            name="residual",
            out_shape=pltpu.VMEM((points, spec_rows, node_count), jnp.float32),
            in_specs=[pl.BlockSpec(memory_space=pltpu.HBM)] * 11,
            out_specs=pl.BlockSpec(memory_space=pltpu.VMEM),
            scratch_shapes=[
                pltpu.SMEM((halo_count, n_node), jnp.int32),
                pltpu.SMEM((listed, block_count), jnp.int32),
                *[pltpu.VMEM((block_count, block_size), jnp.float32)] * 4,
                pltpu.VMEM((rows, rows), jnp.bfloat16),
                pltpu.VMEM((rows, 2 * rows), jnp.bfloat16),
                pltpu.VMEM((points, spec_rows, node_count), jnp.float32),
                pltpu.VMEM((points, spec_rows, node_count), jnp.float32),
                pltpu.VMEM(coupling.shape, jnp.bfloat16),
                pltpu.VMEM((block_count + halo_count + 1, *block), jnp.bfloat16),
                pltpu.VMEM((halo_count, *block), jnp.bfloat16),
                pltpu.VMEM((halo_count, *block), jnp.bfloat16),
                *[pltpu.VMEM((block_count, *block), jnp.bfloat16)] * 3,
                dma((9,)),
                dma((CHUNKS,)),
                dma((COUPLING_COPIES,)),
                dma((len(OFFSETS),)),
                dma((len(OFFSETS),)),
                dma,
                dma((CHUNKS,)),
                dma,
                dma((CHUNKS,)),
                pltpu.SemaphoreType.REGULAR,
                pltpu.SemaphoreType.REGULAR,
                pltpu.VMEM((block_count, *block), jnp.bfloat16),
                pltpu.VMEM((block_count, *block), jnp.bfloat16),
                dma((CHUNKS + 1,)),
            ],
            compiler_params=pltpu.CompilerParams(
                collective_id=0, has_side_effects=True, vmem_limit_bytes=40 * 2**20
            ),
        )(
            held(halo_list.transpose(1, 2, 0).reshape(halo_count, n_node)),
            held(neighbour_slot.T),
            held(spectrum.transpose(1, 0, 2)),
            held(source.transpose(1, 0, 2)),
            held(coupling),
            held(capacitance.reshape(block_count, block_size)),
            held(saturation.reshape(block_count, block_size)),
            held(steepness.reshape(block_count, block_size)),
            held(junction.reshape(block_count, block_size)),
            held(jnp.asarray(synthesis, jnp.bfloat16)),
            held(jnp.asarray(analysis, jnp.bfloat16)),
        )
        return result.transpose(1, 0, 2)

    return jax.shard_map(
        local,
        mesh=mesh,
        in_specs=(
            P("harm", None, "node"),
            P("harm", None, "node"),
            P("node", None, None, None),
            P("node"),
            P("node"),
            P("node"),
            P("node"),
            P(),
            P("node", None),
        ),
        out_specs=P("harm", None, "node"),
        check_vma=False,
    )
```

```python
import functools

import jax
import jax.numpy as jnp
import numpy as np
from jax import lax
from jax.experimental import pallas as pl
from jax.experimental.pallas import tpu as pltpu
from jax.sharding import PartitionSpec as P

OFFSETS = (-2, -1, 1, 2)
LOG2_E = 1.4426950408889634
LN_2 = 0.6931471805599453
MESH = pl.DeviceIdType.MESH
PIECES = (1, 1, 2, 2)
CHUNKS = len(PIECES)
COUPLING_PARTS = 6
EARLY_PARTS = 3
Y_SIZE = 8


def tables(rows):
    time = np.arange(rows)[:, None]
    row = np.arange(rows)[None, :]
    phase = (row // 2) * time % rows
    angle = 2.0 * np.pi / rows * phase
    synthesis = np.where(row % 2 == 1, np.sin(angle), np.cos(angle))
    synthesis = np.where(row == 1, np.where(time % 2 == 0, 1.0, -1.0), synthesis)
    weights = np.where(np.arange(rows) < 2, 1.0 / rows, 2.0 / rows)
    analysis = synthesis.T * weights[:, None]
    pulsation = (np.arange(rows) // 2)[:, None] / (rows // 2)
    derived = np.empty_like(analysis)
    derived[0::2] = pulsation[0::2] * analysis[1::2]
    derived[1::2] = -pulsation[1::2] * analysis[0::2]
    return synthesis, np.concatenate([analysis, derived], axis=1)


def body(
    n_node,
    n_harm,
    halo_hbm,
    slot_hbm,
    spectrum_hbm,
    source_hbm,
    coupling_hbm,
    capacitance_hbm,
    saturation_hbm,
    steepness_hbm,
    junction_hbm,
    synthesis_hbm,
    analysis_hbm,
    out_ref,
    halo_ref,
    slot_ref,
    capacitance_ref,
    saturation_ref,
    steepness_ref,
    junction_ref,
    synthesis_ref,
    analysis_ref,
    spectrum_ref,
    source_ref,
    coupling_ref,
    blocks_ref,
    halo_out_ref,
    halo_in_ref,
    columns_ref,
    back_ref,
    result_ref,
    small_sem,
    spectrum_sem,
    coupling_sem,
    halo_send_sem,
    halo_recv_sem,
    there_send_sem,
    there_recv_sem,
    back_send_sem,
    back_recv_sem,
    node_sem,
    late_sem,
    proxy_ref,
    proxy_back_ref,
    proxy_sem,
):
    node = lax.axis_index("node")
    harm = lax.axis_index("harm")
    points, spec_rows, _ = spectrum_ref.shape
    block_count, listed, block_size, _ = coupling_ref.shape
    share = block_count // n_harm
    starts = [n_harm * sum(PIECES[:c]) for c in range(CHUNKS + 1)]

    def blocks_of(c, owner):
        return pl.ds(starts[c] + owner * PIECES[c], PIECES[c])

    rows = n_harm * spec_rows
    slots = halo_out_ref.shape[0] // len(OFFSETS)
    chips = n_harm // 2
    turns = [(0, 1)] + [(ahead, core) for core in (0, 1) for ahead in (2, 3, 1)]
    peers = [
        lax.rem(harm // 2 + ahead, chips) * 2 + lax.rem(harm + core, 2) for ahead, core in turns
    ]
    neighbours = [node + offset for offset in OFFSETS]

    last = (node == 0) & (harm == 0)
    with_last = (node == 0) & (harm > 0)
    proxy = (node == 0) & (harm == 1)

    middle = n_node // Y_SIZE // 2
    halves = lax.rem(harm // 2, 2) == 1

    def upper_follows(lower, distance):
        y, above = lax.rem(lower, Y_SIZE), lower // Y_SIZE + 1
        low_off = 2 * y - Y_SIZE - 1
        high_off = 2 * lax.rem(y + distance, Y_SIZE) - Y_SIZE - 1
        crosses = y + distance >= Y_SIZE
        across = (above == middle) & halves
        if distance == 2:
            far = y == Y_SIZE - 1
            across = across | ((above < middle) & far & halves) | ((above == middle) & far)
        along = high_off * high_off <= low_off * low_off
        return (crosses & across) | (~crosses & along)

    later, earlier = [], []
    for to, offset in zip(neighbours, OFFSETS):
        on_mesh = (to >= 0) & (to < n_node)
        follows = upper_follows(node, offset) if offset > 0 else ~upper_follows(to, -offset)
        follows = ((to == 0) & (harm == 0)) | (follows & ~last)
        later.append(on_mesh & follows)
        earlier.append(on_mesh & ~follows)

    def count(flags):
        return sum(flag.astype(jnp.int32) for flag in flags)

    load_spectrum = []
    for c in range(CHUNKS):
        at = pl.ds(starts[c] * block_size, (starts[c + 1] - starts[c]) * block_size)
        load_spectrum.append(
            pltpu.make_async_copy(
                spectrum_hbm.at[:, :, at], spectrum_ref.at[:, :, at], spectrum_sem.at[c]
            )
        )
    for copy in load_spectrum:
        copy.start()
    barrier = pltpu.get_barrier_semaphore()

    @pl.when(~last)
    def _():
        for peer in peers:
            pl.semaphore_signal(barrier, inc=1, device_id=(node, peer), device_id_type=MESH)

    for neighbour, flag in zip(neighbours, later):

        @pl.when(flag)
        def _(neighbour=neighbour):
            pl.semaphore_signal(barrier, inc=1, device_id=(neighbour, harm), device_id_type=MESH)

    whole = [
        (halo_hbm, halo_ref),
        (synthesis_hbm, synthesis_ref),
        (analysis_hbm, analysis_ref),
        (saturation_hbm, saturation_ref),
        (steepness_hbm, steepness_ref),
        (junction_hbm, junction_ref),
        (slot_hbm, slot_ref),
        (capacitance_hbm, capacitance_ref),
        (source_hbm, source_ref),
    ]
    loads = [
        pltpu.make_async_copy(source, target, small_sem.at[i])
        for i, (source, target) in enumerate(whole)
    ]
    load_halo, for_nonlinear, for_linear = loads[0], loads[1:6], loads[6:]
    load_halo.start()
    for copy in for_nonlinear:
        copy.start()
    per_part = block_count // COUPLING_PARTS
    load_coupling = pltpu.make_async_copy(coupling_hbm, coupling_ref, coupling_sem)

    def columns_of(b):
        return pl.ds(pl.multiple_of(b * block_size, block_size), block_size)

    def round_block(b, carry):
        blocks_ref[b] = spectrum_ref[:, :, columns_of(b)].astype(jnp.bfloat16)
        return carry

    there_chunks = [
        [
            pltpu.make_async_remote_copy(
                src_ref=blocks_ref.at[blocks_of(c, peer)],
                dst_ref=columns_ref.at[blocks_of(c, harm)],
                send_sem=there_send_sem,
                recv_sem=there_recv_sem.at[c],
                device_id=(node, peer),
                device_id_type=MESH,
            )
            for peer in peers
        ]
        for c in range(CHUNKS)
    ]
    for c in range(CHUNKS):
        with jax.named_scope(f"spectrum_wait_{c}"):
            load_spectrum[c].wait()
        lax.fori_loop(starts[c], starts[c + 1], round_block, 0, unroll=8)
        if c == 0:
            with jax.named_scope("greeting"):
                pl.semaphore_wait(
                    barrier, n_harm - 1 - with_last.astype(jnp.int32) + count(earlier)
                )

        for peer, copy in zip(peers, there_chunks[c]):
            pl.when(~(with_last & (peer == 0)))(copy.start)

        @pl.when((node == 0) & ~proxy)
        def _(c=c):
            pltpu.make_async_remote_copy(
                src_ref=blocks_ref.at[blocks_of(c, 0)],
                dst_ref=proxy_ref.at[blocks_of(c, harm)],
                send_sem=there_send_sem,
                recv_sem=proxy_sem.at[c],
                device_id=(node, 1),
                device_id_type=MESH,
            ).start()

    @pl.when(last)
    def _():
        for peer in peers:
            pl.semaphore_signal(late_sem, inc=1, device_id=(node, peer), device_id_type=MESH)

    for neighbour, flag in zip(neighbours, earlier):

        @pl.when(flag)
        def _(neighbour=neighbour):
            pl.semaphore_signal(node_sem, inc=1, device_id=(neighbour, harm), device_id_type=MESH)

    load_halo.wait()
    for i in range(len(OFFSETS) * slots):
        halo_out_ref[i] = blocks_ref[halo_ref[i, node]]
    empty = block_count + len(OFFSETS) * slots
    blocks_ref[empty] = jnp.zeros(blocks_ref.shape[1:], jnp.bfloat16)
    halo = [
        pltpu.make_async_remote_copy(
            src_ref=halo_out_ref.at[pl.ds(j * slots, slots)],
            dst_ref=halo_in_ref.at[pl.ds(j * slots, slots)],
            send_sem=halo_send_sem.at[j],
            recv_sem=halo_recv_sem.at[j],
            device_id=(neighbour, harm),
            device_id_type=MESH,
        )
        for j, neighbour in enumerate(neighbours)
    ]
    for copy, flag in zip(halo, earlier):
        pl.when(flag)(copy.start)
    for copy in [*for_linear, load_coupling]:
        copy.start()
    for c in range(CHUNKS):
        columns_ref[blocks_of(c, harm)] = blocks_ref[blocks_of(c, harm)]

    @pl.when(proxy)
    def _():
        for c in range(CHUNKS):
            proxy_ref[blocks_of(c, 1)] = blocks_ref[blocks_of(c, 0)]

    for copy in for_nonlinear:
        copy.wait()

    def bytes_of(buffer, blocks, sem):
        part = buffer.at[pl.ds(0, blocks)]
        return pltpu.make_async_copy(part, part, sem)

    def evaluate(row, read, write):
        taken = jnp.concatenate(
            [jnp.concatenate([read(q, p) for q in range(n_harm)], axis=0) for p in range(points)],
            axis=1,
        )
        voltage = jnp.dot(synthesis_ref[...], taken, preferred_element_type=jnp.float32)

        def wide(values):
            return jnp.concatenate([values] * points, axis=1)

        steep = wide(steepness_ref[row] * LOG2_E)
        scale = wide(saturation_ref[row] * LN_2)
        junction = wide(junction_ref[row])
        drive = steep * voltage
        current = scale * (
            jnp.maximum(drive, 0.0) + jnp.log(1.0 + jnp.exp2(-jnp.abs(drive))) * LOG2_E - 1.0
        )
        charge = junction * voltage * lax.rsqrt(1.0 + voltage * voltage)
        both = jnp.concatenate([current.astype(jnp.bfloat16), charge.astype(jnp.bfloat16)], axis=0)
        combined = jnp.dot(analysis_ref[...], both, preferred_element_type=jnp.float32)
        combined = combined.astype(jnp.bfloat16)
        for q in range(n_harm):
            for p in range(points):
                write(
                    q,
                    p,
                    combined[
                        q * spec_rows : (q + 1) * spec_rows,
                        p * block_size : (p + 1) * block_size,
                    ],
                )

    def give(c, owner, given_ref, peer, send_sem):
        return pltpu.make_async_remote_copy(
            src_ref=given_ref.at[blocks_of(c, peer)],
            dst_ref=result_ref.at[blocks_of(c, owner)],
            send_sem=send_sem,
            recv_sem=back_recv_sem.at[c],
            device_id=(node, peer),
            device_id_type=MESH,
        )

    deferring = (node == 0) & (harm > 1)

    def evaluate_chunk(c, owner, taken_ref, given_ref, send_sem):
        for i in range(PIECES[c]):

            def read(q, p):
                return taken_ref[starts[c] + q * PIECES[c] + i, p]

            def write(q, p, values):
                given_ref[starts[c] + q * PIECES[c] + i, p] = values

            evaluate(pl.ds(starts[c] + owner * PIECES[c] + i, 1), read, write)
        order = [(peer, ~(deferring & (peer == 0))) for peer in peers]
        if c >= CHUNKS - 2:
            order = [(1, harm != 1), (0, (harm != 0) & ~deferring)] + [
                (peer, peer > 1) for peer in peers
            ]
        for peer, flag in order:
            pl.when(flag)(give(c, owner, given_ref, peer, send_sem).start)
        result_ref[blocks_of(c, owner)] = given_ref[blocks_of(c, harm)]

    def nonlinear(c):
        with jax.named_scope(f"there_wait_{c}"):
            bytes_of(columns_ref, (n_harm - 1) * PIECES[c], there_recv_sem.at[c]).wait()
        if c == 0:

            @pl.when(with_last)
            def _():
                with jax.named_scope("last_wait"):
                    pl.semaphore_wait(late_sem, 1)

        evaluate_chunk(c, harm, columns_ref, back_ref, back_send_sem)

        @pl.when(proxy)
        def _():
            with jax.named_scope(f"proxy_wait_{c}"):
                bytes_of(proxy_ref, (n_harm - 1) * PIECES[c], proxy_sem.at[c]).wait()
            evaluate_chunk(c, 0, proxy_ref, proxy_back_ref, proxy_sem.at[CHUNKS])

    row_index = lax.broadcasted_iota(jnp.int32, (1, 8, block_size), 1)
    even = row_index % 2 == 0
    tiles = spec_rows // 8
    pulsations = []
    for i in range(tiles):
        harmonic = (harm * spec_rows + i * 8 + row_index) // 2
        value = harmonic.astype(jnp.float32) * (2.0 / rows)
        pulsations.append(jnp.where(even, value, -value))
    pulsation = jnp.concatenate(pulsations * points, axis=0)

    def couple(b, carry):
        gathered = jnp.concatenate(
            [
                blocks_ref[slot_ref[k, b]].reshape(points * spec_rows, block_size)
                for k in range(listed)
            ],
            axis=1,
        )
        matrix = jnp.concatenate([coupling_ref[b, k] for k in range(listed)], axis=1)
        coupled = lax.dot_general(
            gathered, matrix, (((1,), (1,)), ((), ())), preferred_element_type=jnp.float32
        )
        columns = columns_of(b)
        stored = capacitance_ref[pl.ds(b, 1)] * spectrum_ref[:, :, columns].reshape(
            points * spec_rows, block_size
        )
        stored = stored.reshape(points * tiles, 8, block_size)
        swapped = jnp.where(even, pltpu.roll(stored, 7, 1), pltpu.roll(stored, 1, 1))
        linear = (pulsation * swapped).reshape(points, spec_rows, block_size)
        out_ref[:, :, columns] = (
            coupled.reshape(points, spec_rows, block_size) + linear - source_ref[:, :, columns]
        )
        return carry

    with jax.named_scope("node_wait"):
        awaited = count(later)

        @pl.when(awaited > 0)
        def _():
            pl.semaphore_wait(node_sem, awaited)

    for copy, flag in zip(halo, later):
        pl.when(flag)(copy.start)

    def take_halo():
        with jax.named_scope("halo_wait"):
            for j, copy in enumerate(halo):
                opposite = len(OFFSETS) - 1 - j
                pl.when(later[opposite] | earlier[opposite])(copy.wait_recv)
        blocks_ref[pl.ds(block_count, len(OFFSETS) * slots)] = halo_in_ref[...]
        for copy in [*for_linear, load_coupling]:
            copy.wait()

    def couple_part(part, carry):
        first = part * per_part
        for i in range(per_part):
            couple(first + i, 0)
        return carry

    early = jnp.where(proxy, EARLY_PARTS, 0)

    @pl.when(proxy)
    def _():
        take_halo()
        with jax.named_scope("couple_early"):
            lax.fori_loop(0, EARLY_PARTS, couple_part, 0)

    @pl.when(~last)
    def _():
        for c in range(CHUNKS):
            nonlinear(c)

        @pl.when(deferring)
        def _():
            for c in range(CHUNKS):
                give(c, harm, back_ref, 0, back_send_sem).start()

    pl.when(~proxy)(take_halo)
    with jax.named_scope("couple"):
        lax.fori_loop(early, COUPLING_PARTS, couple_part, 0)

    def wait_blocks(flag, buffer, blocks, sem):
        pl.when(flag)(lambda: bytes_of(buffer, blocks, sem).wait())

    plain = ~last & ~proxy
    for c in range(CHUNKS):
        with jax.named_scope(f"back_wait_{c}"):
            wait_blocks(plain, result_ref, (n_harm - 1) * PIECES[c], back_recv_sem.at[c])
            wait_blocks(proxy, result_ref, (n_harm - 2) * PIECES[c], back_recv_sem.at[c])
            wait_blocks(last, result_ref, n_harm * PIECES[c], back_recv_sem.at[c])
        if c == CHUNKS - 1:
            with jax.named_scope("sent"):
                for copy, up, down in zip(halo, later, earlier):
                    pl.when(up | down)(copy.wait_send)
                wait_blocks(plain, blocks_ref, (n_harm - 1) * share, there_send_sem)
                wait_blocks(proxy, blocks_ref, (n_harm - 2) * share, there_send_sem)
                wait_blocks(last, blocks_ref, n_harm * share, there_send_sem)
                wait_blocks(~last, back_ref, (n_harm - 1) * share, back_send_sem)
                wait_blocks(proxy, back_ref, (n_harm - 1) * share, proxy_sem.at[CHUNKS])
        with jax.named_scope(f"add_{c}"):
            for b in range(starts[c], starts[c + 1]):
                at = pl.ds(b * block_size, block_size)
                out_ref[:, :, at] += result_ref[b].astype(jnp.float32)


def solution(mesh):
    n_node, n_harm = mesh.shape["node"], mesh.shape["harm"]

    def local(
        spectrum,
        source,
        coupling,
        capacitance,
        saturation,
        steepness,
        junction,
        halo_list,
        neighbour_slot,
    ):
        spec_rows, points, node_count = spectrum.shape
        block_count, listed, block_size, _ = coupling.shape
        rows = spec_rows * n_harm
        slots = halo_list.shape[2]
        synthesis, analysis = tables(rows)
        halo_count = len(OFFSETS) * slots
        block = (points, spec_rows, block_size)
        held = functools.partial(pltpu.with_memory_space_constraint, memory_space=pltpu.HBM)
        dma = pltpu.SemaphoreType.DMA
        result = pl.pallas_call(
            functools.partial(body, n_node, n_harm),
            name="residual",
            out_shape=pltpu.VMEM((points, spec_rows, node_count), jnp.float32),
            in_specs=[pl.BlockSpec(memory_space=pltpu.HBM)] * 11,
            out_specs=pl.BlockSpec(memory_space=pltpu.VMEM),
            scratch_shapes=[
                pltpu.SMEM((halo_count, n_node), jnp.int32),
                pltpu.SMEM((listed, block_count), jnp.int32),
                *[pltpu.VMEM((block_count, block_size), jnp.float32)] * 4,
                pltpu.VMEM((rows, rows), jnp.bfloat16),
                pltpu.VMEM((rows, 2 * rows), jnp.bfloat16),
                pltpu.VMEM((points, spec_rows, node_count), jnp.float32),
                pltpu.VMEM((points, spec_rows, node_count), jnp.float32),
                pltpu.VMEM(coupling.shape, jnp.bfloat16),
                pltpu.VMEM((block_count + halo_count + 1, *block), jnp.bfloat16),
                pltpu.VMEM((halo_count, *block), jnp.bfloat16),
                pltpu.VMEM((halo_count, *block), jnp.bfloat16),
                *[pltpu.VMEM((block_count, *block), jnp.bfloat16)] * 3,
                dma((9,)),
                dma((CHUNKS,)),
                dma,
                dma((len(OFFSETS),)),
                dma((len(OFFSETS),)),
                dma,
                dma((CHUNKS,)),
                dma,
                dma((CHUNKS,)),
                pltpu.SemaphoreType.REGULAR,
                pltpu.SemaphoreType.REGULAR,
                pltpu.VMEM((block_count, *block), jnp.bfloat16),
                pltpu.VMEM((block_count, *block), jnp.bfloat16),
                dma((CHUNKS + 1,)),
            ],
            compiler_params=pltpu.CompilerParams(
                collective_id=0, has_side_effects=True, vmem_limit_bytes=40 * 2**20
            ),
        )(
            held(halo_list.transpose(1, 2, 0).reshape(halo_count, n_node)),
            held(neighbour_slot.T),
            held(spectrum.transpose(1, 0, 2)),
            held(source.transpose(1, 0, 2)),
            held(coupling),
            held(capacitance.reshape(block_count, block_size)),
            held(saturation.reshape(block_count, block_size)),
            held(steepness.reshape(block_count, block_size)),
            held(junction.reshape(block_count, block_size)),
            held(jnp.asarray(synthesis, jnp.bfloat16)),
            held(jnp.asarray(analysis, jnp.bfloat16)),
        )
        return result.transpose(1, 0, 2)

    return jax.shard_map(
        local,
        mesh=mesh,
        in_specs=(
            P("harm", None, "node"),
            P("harm", None, "node"),
            P("node", None, None, None),
            P("node"),
            P("node"),
            P("node"),
            P("node"),
            P(),
            P("node", None),
        ),
        out_specs=P("harm", None, "node"),
        check_vma=False,
    )
```

```python
import functools

import jax
import jax.numpy as jnp
import numpy as np
from jax import lax
from jax.experimental import pallas as pl
from jax.experimental.pallas import tpu as pltpu
from jax.sharding import PartitionSpec as P

OFFSETS = (-2, -1, 1, 2)
LOG2_E = 1.4426950408889634
LN_2 = 0.6931471805599453
MESH = pl.DeviceIdType.MESH
PIECES = (1, 1, 2, 2)
CHUNKS = len(PIECES)
COUPLING_PARTS = 6
EARLY_PARTS = 3
Y_SIZE = 8


def tables(rows):
    time = np.arange(rows)[:, None]
    row = np.arange(rows)[None, :]
    phase = (row // 2) * time % rows
    angle = 2.0 * np.pi / rows * phase
    synthesis = np.where(row % 2 == 1, np.sin(angle), np.cos(angle))
    synthesis = np.where(row == 1, np.where(time % 2 == 0, 1.0, -1.0), synthesis)
    weights = np.where(np.arange(rows) < 2, 1.0 / rows, 2.0 / rows)
    analysis = synthesis.T * weights[:, None]
    pulsation = (np.arange(rows) // 2)[:, None] / (rows // 2)
    derived = np.empty_like(analysis)
    derived[0::2] = pulsation[0::2] * analysis[1::2]
    derived[1::2] = -pulsation[1::2] * analysis[0::2]
    return synthesis, np.concatenate([analysis, derived], axis=1)


def body(
    n_node,
    n_harm,
    halo_hbm,
    slot_hbm,
    spectrum_hbm,
    source_hbm,
    coupling_hbm,
    capacitance_hbm,
    saturation_hbm,
    steepness_hbm,
    junction_hbm,
    synthesis_hbm,
    analysis_hbm,
    out_ref,
    halo_ref,
    slot_ref,
    capacitance_ref,
    saturation_ref,
    steepness_ref,
    junction_ref,
    synthesis_ref,
    analysis_ref,
    spectrum_ref,
    source_ref,
    coupling_ref,
    blocks_ref,
    halo_out_ref,
    halo_in_ref,
    columns_ref,
    back_ref,
    result_ref,
    small_sem,
    spectrum_sem,
    coupling_sem,
    halo_send_sem,
    halo_recv_sem,
    there_send_sem,
    there_recv_sem,
    back_send_sem,
    back_recv_sem,
    node_sem,
    late_sem,
    proxy_ref,
    proxy_back_ref,
    proxy_sem,
):
    node = lax.axis_index("node")
    harm = lax.axis_index("harm")
    points, spec_rows, _ = spectrum_ref.shape
    block_count, listed, block_size, _ = coupling_ref.shape
    share = block_count // n_harm
    starts = [n_harm * sum(PIECES[:c]) for c in range(CHUNKS + 1)]

    def blocks_of(c, owner):
        return pl.ds(starts[c] + owner * PIECES[c], PIECES[c])

    rows = n_harm * spec_rows
    slots = halo_out_ref.shape[0] // len(OFFSETS)
    chips = n_harm // 2
    turns = [(0, 1)] + [(ahead, core) for core in (0, 1) for ahead in (2, 3, 1)]
    peers = [
        lax.rem(harm // 2 + ahead, chips) * 2 + lax.rem(harm + core, 2) for ahead, core in turns
    ]
    neighbours = [node + offset for offset in OFFSETS]

    last = (node == 0) & (harm == 0)
    with_last = (node == 0) & (harm > 0)
    proxy = (node == 0) & (harm == 1)

    middle = n_node // Y_SIZE // 2
    halves = lax.rem(harm // 2, 2) == 1

    def upper_follows(lower, distance):
        y, above = lax.rem(lower, Y_SIZE), lower // Y_SIZE + 1
        low_off = 2 * y - Y_SIZE - 1
        high_off = 2 * lax.rem(y + distance, Y_SIZE) - Y_SIZE - 1
        crosses = y + distance >= Y_SIZE
        across = (above == middle) & halves
        if distance == 2:
            far = y == Y_SIZE - 1
            across = across | ((above < middle) & far & halves) | ((above == middle) & far)
        along = high_off * high_off <= low_off * low_off
        return (crosses & across) | (~crosses & along)

    later, earlier = [], []
    for to, offset in zip(neighbours, OFFSETS):
        on_mesh = (to >= 0) & (to < n_node)
        follows = upper_follows(node, offset) if offset > 0 else ~upper_follows(to, -offset)
        follows = ((to == 0) & (harm == 0)) | (follows & ~last)
        later.append(on_mesh & follows)
        earlier.append(on_mesh & ~follows)

    def count(flags):
        return sum(flag.astype(jnp.int32) for flag in flags)

    load_spectrum = []
    for c in range(CHUNKS):
        at = pl.ds(starts[c] * block_size, (starts[c + 1] - starts[c]) * block_size)
        load_spectrum.append(
            pltpu.make_async_copy(
                spectrum_hbm.at[:, :, at], spectrum_ref.at[:, :, at], spectrum_sem.at[c]
            )
        )
    load_spectrum[0].start()
    barrier = pltpu.get_barrier_semaphore()

    @pl.when(~last)
    def _():
        for peer in peers:
            pl.semaphore_signal(barrier, inc=1, device_id=(node, peer), device_id_type=MESH)

    for neighbour, flag in zip(neighbours, later):

        @pl.when(flag)
        def _(neighbour=neighbour):
            pl.semaphore_signal(barrier, inc=1, device_id=(neighbour, harm), device_id_type=MESH)

    for copy in load_spectrum[1:]:
        copy.start()
    whole = [
        (halo_hbm, halo_ref),
        (synthesis_hbm, synthesis_ref),
        (analysis_hbm, analysis_ref),
        (saturation_hbm, saturation_ref),
        (steepness_hbm, steepness_ref),
        (junction_hbm, junction_ref),
        (slot_hbm, slot_ref),
        (capacitance_hbm, capacitance_ref),
        (source_hbm, source_ref),
    ]
    loads = [
        pltpu.make_async_copy(source, target, small_sem.at[i])
        for i, (source, target) in enumerate(whole)
    ]
    load_halo, for_nonlinear, for_linear = loads[0], loads[1:6], loads[6:]
    load_halo.start()
    for copy in for_nonlinear:
        copy.start()
    per_part = block_count // COUPLING_PARTS
    load_coupling = pltpu.make_async_copy(coupling_hbm, coupling_ref, coupling_sem)

    def columns_of(b):
        return pl.ds(pl.multiple_of(b * block_size, block_size), block_size)

    def round_block(b, carry):
        blocks_ref[b] = spectrum_ref[:, :, columns_of(b)].astype(jnp.bfloat16)
        return carry

    there_chunks = [
        [
            pltpu.make_async_remote_copy(
                src_ref=blocks_ref.at[blocks_of(c, peer)],
                dst_ref=columns_ref.at[blocks_of(c, harm)],
                send_sem=there_send_sem,
                recv_sem=there_recv_sem.at[c],
                device_id=(node, peer),
                device_id_type=MESH,
            )
            for peer in peers
        ]
        for c in range(CHUNKS)
    ]
    for c in range(CHUNKS):
        with jax.named_scope(f"spectrum_wait_{c}"):
            load_spectrum[c].wait()
        lax.fori_loop(starts[c], starts[c + 1], round_block, 0, unroll=8)
        if c == 0:
            with jax.named_scope("greeting"):
                pl.semaphore_wait(
                    barrier, n_harm - 1 - with_last.astype(jnp.int32) + count(earlier)
                )

        for peer, copy in zip(peers, there_chunks[c]):
            pl.when(~(with_last & (peer == 0)))(copy.start)

        @pl.when((node == 0) & ~proxy)
        def _(c=c):
            pltpu.make_async_remote_copy(
                src_ref=blocks_ref.at[blocks_of(c, 0)],
                dst_ref=proxy_ref.at[blocks_of(c, harm)],
                send_sem=there_send_sem,
                recv_sem=proxy_sem.at[c],
                device_id=(node, 1),
                device_id_type=MESH,
            ).start()

    @pl.when(last)
    def _():
        for peer in peers:
            pl.semaphore_signal(late_sem, inc=1, device_id=(node, peer), device_id_type=MESH)

    for neighbour, flag in zip(neighbours, earlier):

        @pl.when(flag)
        def _(neighbour=neighbour):
            pl.semaphore_signal(node_sem, inc=1, device_id=(neighbour, harm), device_id_type=MESH)

    load_halo.wait()
    for i in range(len(OFFSETS) * slots):
        halo_out_ref[i] = blocks_ref[halo_ref[i, node]]
    empty = block_count + len(OFFSETS) * slots
    blocks_ref[empty] = jnp.zeros(blocks_ref.shape[1:], jnp.bfloat16)
    halo = [
        pltpu.make_async_remote_copy(
            src_ref=halo_out_ref.at[pl.ds(j * slots, slots)],
            dst_ref=halo_in_ref.at[pl.ds(j * slots, slots)],
            send_sem=halo_send_sem.at[j],
            recv_sem=halo_recv_sem.at[j],
            device_id=(neighbour, harm),
            device_id_type=MESH,
        )
        for j, neighbour in enumerate(neighbours)
    ]
    for copy, flag in zip(halo, earlier):
        pl.when(flag)(copy.start)
    for copy in [*for_linear, load_coupling]:
        copy.start()
    for c in range(CHUNKS):
        columns_ref[blocks_of(c, harm)] = blocks_ref[blocks_of(c, harm)]

    @pl.when(proxy)
    def _():
        for c in range(CHUNKS):
            proxy_ref[blocks_of(c, 1)] = blocks_ref[blocks_of(c, 0)]

    for copy in for_nonlinear:
        copy.wait()

    def bytes_of(buffer, blocks, sem):
        part = buffer.at[pl.ds(0, blocks)]
        return pltpu.make_async_copy(part, part, sem)

    def evaluate(row, read, write):
        taken = jnp.concatenate(
            [jnp.concatenate([read(q, p) for q in range(n_harm)], axis=0) for p in range(points)],
            axis=1,
        )
        voltage = jnp.dot(synthesis_ref[...], taken, preferred_element_type=jnp.float32)

        def wide(values):
            return jnp.concatenate([values] * points, axis=1)

        steep = wide(steepness_ref[row] * LOG2_E)
        scale = wide(saturation_ref[row] * LN_2)
        junction = wide(junction_ref[row])
        drive = steep * voltage
        current = scale * (
            jnp.maximum(drive, 0.0) + jnp.log(1.0 + jnp.exp2(-jnp.abs(drive))) * LOG2_E - 1.0
        )
        charge = junction * voltage * lax.rsqrt(1.0 + voltage * voltage)
        both = jnp.concatenate([current.astype(jnp.bfloat16), charge.astype(jnp.bfloat16)], axis=0)
        combined = jnp.dot(analysis_ref[...], both, preferred_element_type=jnp.float32)
        combined = combined.astype(jnp.bfloat16)
        for q in range(n_harm):
            for p in range(points):
                write(
                    q,
                    p,
                    combined[
                        q * spec_rows : (q + 1) * spec_rows,
                        p * block_size : (p + 1) * block_size,
                    ],
                )

    def give(c, owner, given_ref, peer, send_sem):
        return pltpu.make_async_remote_copy(
            src_ref=given_ref.at[blocks_of(c, peer)],
            dst_ref=result_ref.at[blocks_of(c, owner)],
            send_sem=send_sem,
            recv_sem=back_recv_sem.at[c],
            device_id=(node, peer),
            device_id_type=MESH,
        )

    deferring = (node == 0) & (harm > 1)

    def evaluate_chunk(c, owner, taken_ref, given_ref, send_sem):
        for i in range(PIECES[c]):

            def read(q, p):
                return taken_ref[starts[c] + q * PIECES[c] + i, p]

            def write(q, p, values):
                given_ref[starts[c] + q * PIECES[c] + i, p] = values

            evaluate(pl.ds(starts[c] + owner * PIECES[c] + i, 1), read, write)
        order = [(peer, ~(deferring & (peer == 0))) for peer in peers]
        if c >= CHUNKS - 2:
            order = [(1, harm != 1), (0, (harm != 0) & ~deferring)] + [
                (peer, peer > 1) for peer in peers
            ]
        for peer, flag in order:
            pl.when(flag)(give(c, owner, given_ref, peer, send_sem).start)
        result_ref[blocks_of(c, owner)] = given_ref[blocks_of(c, harm)]

    def nonlinear(c):
        with jax.named_scope(f"there_wait_{c}"):
            bytes_of(columns_ref, (n_harm - 1) * PIECES[c], there_recv_sem.at[c]).wait()
        if c == 0:

            @pl.when(with_last)
            def _():
                with jax.named_scope("last_wait"):
                    pl.semaphore_wait(late_sem, 1)

        evaluate_chunk(c, harm, columns_ref, back_ref, back_send_sem)

        @pl.when(proxy)
        def _():
            with jax.named_scope(f"proxy_wait_{c}"):
                bytes_of(proxy_ref, (n_harm - 1) * PIECES[c], proxy_sem.at[c]).wait()
            evaluate_chunk(c, 0, proxy_ref, proxy_back_ref, proxy_sem.at[CHUNKS])

    row_index = lax.broadcasted_iota(jnp.int32, (1, 8, block_size), 1)
    even = row_index % 2 == 0
    tiles = spec_rows // 8
    pulsations = []
    for i in range(tiles):
        harmonic = (harm * spec_rows + i * 8 + row_index) // 2
        value = harmonic.astype(jnp.float32) * (2.0 / rows)
        pulsations.append(jnp.where(even, value, -value))
    pulsation = jnp.concatenate(pulsations * points, axis=0)

    def couple(b, carry):
        gathered = jnp.concatenate(
            [
                blocks_ref[slot_ref[k, b]].reshape(points * spec_rows, block_size)
                for k in range(listed)
            ],
            axis=1,
        )
        matrix = jnp.concatenate([coupling_ref[b, k] for k in range(listed)], axis=1)
        coupled = lax.dot_general(
            gathered, matrix, (((1,), (1,)), ((), ())), preferred_element_type=jnp.float32
        )
        columns = columns_of(b)
        stored = capacitance_ref[pl.ds(b, 1)] * spectrum_ref[:, :, columns].reshape(
            points * spec_rows, block_size
        )
        stored = stored.reshape(points * tiles, 8, block_size)
        swapped = jnp.where(even, pltpu.roll(stored, 7, 1), pltpu.roll(stored, 1, 1))
        linear = (pulsation * swapped).reshape(points, spec_rows, block_size)
        out_ref[:, :, columns] = (
            coupled.reshape(points, spec_rows, block_size) + linear - source_ref[:, :, columns]
        )
        return carry

    with jax.named_scope("node_wait"):
        awaited = count(later)

        @pl.when(awaited > 0)
        def _():
            pl.semaphore_wait(node_sem, awaited)

    for copy, flag in zip(halo, later):
        pl.when(flag)(copy.start)

    def take_halo():
        with jax.named_scope("halo_wait"):
            for j, copy in enumerate(halo):
                opposite = len(OFFSETS) - 1 - j
                pl.when(later[opposite] | earlier[opposite])(copy.wait_recv)
        blocks_ref[pl.ds(block_count, len(OFFSETS) * slots)] = halo_in_ref[...]
        for copy in [*for_linear, load_coupling]:
            copy.wait()

    def couple_part(part, carry):
        first = part * per_part
        for i in range(per_part):
            couple(first + i, 0)
        return carry

    early = jnp.where(proxy, EARLY_PARTS, 0)

    @pl.when(proxy)
    def _():
        take_halo()
        with jax.named_scope("couple_early"):
            lax.fori_loop(0, EARLY_PARTS, couple_part, 0)

    @pl.when(~last)
    def _():
        for c in range(CHUNKS):
            nonlinear(c)

        @pl.when(deferring)
        def _():
            for c in range(CHUNKS):
                give(c, harm, back_ref, 0, back_send_sem).start()

    pl.when(~proxy)(take_halo)
    with jax.named_scope("couple"):
        lax.fori_loop(early, COUPLING_PARTS, couple_part, 0)

    def wait_blocks(flag, buffer, blocks, sem):
        pl.when(flag)(lambda: bytes_of(buffer, blocks, sem).wait())

    plain = ~last & ~proxy
    for c in range(CHUNKS):
        with jax.named_scope(f"back_wait_{c}"):
            wait_blocks(plain, result_ref, (n_harm - 1) * PIECES[c], back_recv_sem.at[c])
            wait_blocks(proxy, result_ref, (n_harm - 2) * PIECES[c], back_recv_sem.at[c])
            wait_blocks(last, result_ref, n_harm * PIECES[c], back_recv_sem.at[c])
        if c == CHUNKS - 1:
            with jax.named_scope("sent"):
                for copy, up, down in zip(halo, later, earlier):
                    pl.when(up | down)(copy.wait_send)
                wait_blocks(plain, blocks_ref, (n_harm - 1) * share, there_send_sem)
                wait_blocks(proxy, blocks_ref, (n_harm - 2) * share, there_send_sem)
                wait_blocks(last, blocks_ref, n_harm * share, there_send_sem)
                wait_blocks(~last, back_ref, (n_harm - 1) * share, back_send_sem)
                wait_blocks(proxy, back_ref, (n_harm - 1) * share, proxy_sem.at[CHUNKS])
        with jax.named_scope(f"add_{c}"):
            for b in range(starts[c], starts[c + 1]):
                at = pl.ds(b * block_size, block_size)
                out_ref[:, :, at] += result_ref[b].astype(jnp.float32)


def solution(mesh):
    n_node, n_harm = mesh.shape["node"], mesh.shape["harm"]

    def local(
        spectrum,
        source,
        coupling,
        capacitance,
        saturation,
        steepness,
        junction,
        halo_list,
        neighbour_slot,
    ):
        spec_rows, points, node_count = spectrum.shape
        block_count, listed, block_size, _ = coupling.shape
        rows = spec_rows * n_harm
        slots = halo_list.shape[2]
        synthesis, analysis = tables(rows)
        halo_count = len(OFFSETS) * slots
        block = (points, spec_rows, block_size)
        held = functools.partial(pltpu.with_memory_space_constraint, memory_space=pltpu.HBM)
        dma = pltpu.SemaphoreType.DMA
        result = pl.pallas_call(
            functools.partial(body, n_node, n_harm),
            name="residual",
            out_shape=pltpu.VMEM((points, spec_rows, node_count), jnp.float32),
            in_specs=[pl.BlockSpec(memory_space=pltpu.HBM)] * 11,
            out_specs=pl.BlockSpec(memory_space=pltpu.VMEM),
            scratch_shapes=[
                pltpu.SMEM((halo_count, n_node), jnp.int32),
                pltpu.SMEM((listed, block_count), jnp.int32),
                *[pltpu.VMEM((block_count, block_size), jnp.float32)] * 4,
                pltpu.VMEM((rows, rows), jnp.bfloat16),
                pltpu.VMEM((rows, 2 * rows), jnp.bfloat16),
                pltpu.VMEM((points, spec_rows, node_count), jnp.float32),
                pltpu.VMEM((points, spec_rows, node_count), jnp.float32),
                pltpu.VMEM(coupling.shape, jnp.bfloat16),
                pltpu.VMEM((block_count + halo_count + 1, *block), jnp.bfloat16),
                pltpu.VMEM((halo_count, *block), jnp.bfloat16),
                pltpu.VMEM((halo_count, *block), jnp.bfloat16),
                *[pltpu.VMEM((block_count, *block), jnp.bfloat16)] * 3,
                dma((9,)),
                dma((CHUNKS,)),
                dma,
                dma((len(OFFSETS),)),
                dma((len(OFFSETS),)),
                dma,
                dma((CHUNKS,)),
                dma,
                dma((CHUNKS,)),
                pltpu.SemaphoreType.REGULAR,
                pltpu.SemaphoreType.REGULAR,
                pltpu.VMEM((block_count, *block), jnp.bfloat16),
                pltpu.VMEM((block_count, *block), jnp.bfloat16),
                dma((CHUNKS + 1,)),
            ],
            compiler_params=pltpu.CompilerParams(
                collective_id=0, has_side_effects=True, vmem_limit_bytes=40 * 2**20
            ),
        )(
            held(halo_list.transpose(1, 2, 0).reshape(halo_count, n_node)),
            held(neighbour_slot.T),
            held(spectrum.transpose(1, 0, 2)),
            held(source.transpose(1, 0, 2)),
            held(coupling),
            held(capacitance.reshape(block_count, block_size)),
            held(saturation.reshape(block_count, block_size)),
            held(steepness.reshape(block_count, block_size)),
            held(junction.reshape(block_count, block_size)),
            held(jnp.asarray(synthesis, jnp.bfloat16)),
            held(jnp.asarray(analysis, jnp.bfloat16)),
        )
        return result.transpose(1, 0, 2)

    return jax.shard_map(
        local,
        mesh=mesh,
        in_specs=(
            P("harm", None, "node"),
            P("harm", None, "node"),
            P("node", None, None, None),
            P("node"),
            P("node"),
            P("node"),
            P("node"),
            P(),
            P("node", None),
        ),
        out_specs=P("harm", None, "node"),
        check_vma=False,
    )
```

```python
import functools

import jax
import jax.numpy as jnp
import numpy as np
from jax import lax
from jax.experimental import pallas as pl
from jax.experimental.pallas import tpu as pltpu
from jax.sharding import PartitionSpec as P

OFFSETS = (-2, -1, 1, 2)
LOG2_E = 1.4426950408889634
LN_2 = 0.6931471805599453
MESH = pl.DeviceIdType.MESH
PIECES = (1, 1, 2, 2)
CHUNKS = len(PIECES)
COUPLING_PARTS = 6
EARLY_PARTS = 3
Y_SIZE = 8


def tables(rows):
    time = np.arange(rows)[:, None]
    row = np.arange(rows)[None, :]
    phase = (row // 2) * time % rows
    angle = 2.0 * np.pi / rows * phase
    synthesis = np.where(row % 2 == 1, np.sin(angle), np.cos(angle))
    synthesis = np.where(row == 1, np.where(time % 2 == 0, 1.0, -1.0), synthesis)
    weights = np.where(np.arange(rows) < 2, 1.0 / rows, 2.0 / rows)
    analysis = synthesis.T * weights[:, None]
    pulsation = (np.arange(rows) // 2)[:, None] / (rows // 2)
    derived = np.empty_like(analysis)
    derived[0::2] = pulsation[0::2] * analysis[1::2]
    derived[1::2] = -pulsation[1::2] * analysis[0::2]
    return synthesis, np.concatenate([analysis, derived], axis=1)


def body(
    n_node,
    n_harm,
    halo_hbm,
    slot_hbm,
    spectrum_hbm,
    source_hbm,
    coupling_hbm,
    capacitance_hbm,
    saturation_hbm,
    steepness_hbm,
    junction_hbm,
    synthesis_hbm,
    analysis_hbm,
    out_ref,
    halo_ref,
    slot_ref,
    capacitance_ref,
    saturation_ref,
    steepness_ref,
    junction_ref,
    synthesis_ref,
    analysis_ref,
    spectrum_ref,
    source_ref,
    coupling_ref,
    blocks_ref,
    halo_out_ref,
    halo_in_ref,
    columns_ref,
    back_ref,
    result_ref,
    small_sem,
    spectrum_sem,
    coupling_sem,
    halo_send_sem,
    halo_recv_sem,
    there_send_sem,
    there_recv_sem,
    back_send_sem,
    back_recv_sem,
    node_sem,
    late_sem,
    proxy_ref,
    proxy_back_ref,
    proxy_sem,
):
    node = lax.axis_index("node")
    harm = lax.axis_index("harm")
    points, spec_rows, _ = spectrum_ref.shape
    block_count, listed, block_size, _ = coupling_ref.shape
    share = block_count // n_harm
    starts = [n_harm * sum(PIECES[:c]) for c in range(CHUNKS + 1)]

    def blocks_of(c, owner):
        return pl.ds(starts[c] + owner * PIECES[c], PIECES[c])

    rows = n_harm * spec_rows
    slots = halo_out_ref.shape[0] // len(OFFSETS)
    chips = n_harm // 2
    turns = [(0, 1)] + [(ahead, core) for core in (0, 1) for ahead in (2, 3, 1)]
    peers = [
        lax.rem(harm // 2 + ahead, chips) * 2 + lax.rem(harm + core, 2) for ahead, core in turns
    ]
    neighbours = [node + offset for offset in OFFSETS]

    last = (node == 0) & (harm == 0)
    with_last = (node == 0) & (harm > 0)
    proxy = (node == 0) & (harm == 1)

    middle = n_node // Y_SIZE // 2
    halves = lax.rem(harm // 2, 2) == 1

    def upper_follows(lower, distance):
        y, above = lax.rem(lower, Y_SIZE), lower // Y_SIZE + 1
        low_off = 2 * y - Y_SIZE - 1
        high_off = 2 * lax.rem(y + distance, Y_SIZE) - Y_SIZE - 1
        crosses = y + distance >= Y_SIZE
        across = (above == middle) & halves
        if distance == 2:
            far = y == Y_SIZE - 1
            across = across | ((above < middle) & far & halves) | ((above == middle) & far)
        along = high_off * high_off <= low_off * low_off
        return (crosses & across) | (~crosses & along)

    later, earlier = [], []
    for to, offset in zip(neighbours, OFFSETS):
        on_mesh = (to >= 0) & (to < n_node)
        follows = upper_follows(node, offset) if offset > 0 else ~upper_follows(to, -offset)
        follows = ((to == 0) & (harm == 0)) | (follows & ~last)
        later.append(on_mesh & follows)
        earlier.append(on_mesh & ~follows)

    def count(flags):
        return sum(flag.astype(jnp.int32) for flag in flags)

    load_spectrum = []
    for c in range(CHUNKS):
        at = pl.ds(starts[c] * block_size, (starts[c + 1] - starts[c]) * block_size)
        load_spectrum.append(
            pltpu.make_async_copy(
                spectrum_hbm.at[:, :, at], spectrum_ref.at[:, :, at], spectrum_sem.at[c]
            )
        )
    load_spectrum[0].start()
    barrier = pltpu.get_barrier_semaphore()

    for neighbour, flag in zip(neighbours, later):

        @pl.when(flag)
        def _(neighbour=neighbour):
            pl.semaphore_signal(barrier, inc=1, device_id=(neighbour, harm), device_id_type=MESH)

    @pl.when(~last)
    def _():
        for peer in peers:
            pl.semaphore_signal(barrier, inc=1, device_id=(node, peer), device_id_type=MESH)

    for copy in load_spectrum[1:]:
        copy.start()
    whole = [
        (halo_hbm, halo_ref),
        (synthesis_hbm, synthesis_ref),
        (analysis_hbm, analysis_ref),
        (saturation_hbm, saturation_ref),
        (steepness_hbm, steepness_ref),
        (junction_hbm, junction_ref),
        (slot_hbm, slot_ref),
        (capacitance_hbm, capacitance_ref),
        (source_hbm, source_ref),
    ]
    loads = [
        pltpu.make_async_copy(source, target, small_sem.at[i])
        for i, (source, target) in enumerate(whole)
    ]
    load_halo, for_nonlinear, for_linear = loads[0], loads[1:6], loads[6:]
    load_halo.start()
    for copy in for_nonlinear:
        copy.start()
    per_part = block_count // COUPLING_PARTS
    load_coupling = pltpu.make_async_copy(coupling_hbm, coupling_ref, coupling_sem)

    def columns_of(b):
        return pl.ds(pl.multiple_of(b * block_size, block_size), block_size)

    def round_block(b, carry):
        blocks_ref[b] = spectrum_ref[:, :, columns_of(b)].astype(jnp.bfloat16)
        return carry

    there_chunks = [
        [
            pltpu.make_async_remote_copy(
                src_ref=blocks_ref.at[blocks_of(c, peer)],
                dst_ref=columns_ref.at[blocks_of(c, harm)],
                send_sem=there_send_sem,
                recv_sem=there_recv_sem.at[c],
                device_id=(node, peer),
                device_id_type=MESH,
            )
            for peer in peers
        ]
        for c in range(CHUNKS)
    ]
    for c in range(CHUNKS):
        with jax.named_scope(f"spectrum_wait_{c}"):
            load_spectrum[c].wait()
        lax.fori_loop(starts[c], starts[c + 1], round_block, 0, unroll=8)
        if c == 0:
            with jax.named_scope("greeting"):
                pl.semaphore_wait(
                    barrier, n_harm - 1 - with_last.astype(jnp.int32) + count(earlier)
                )

        for peer, copy in zip(peers, there_chunks[c]):
            pl.when(~(with_last & (peer == 0)))(copy.start)

        @pl.when((node == 0) & ~proxy)
        def _(c=c):
            pltpu.make_async_remote_copy(
                src_ref=blocks_ref.at[blocks_of(c, 0)],
                dst_ref=proxy_ref.at[blocks_of(c, harm)],
                send_sem=there_send_sem,
                recv_sem=proxy_sem.at[c],
                device_id=(node, 1),
                device_id_type=MESH,
            ).start()

    @pl.when(last)
    def _():
        for peer in peers:
            pl.semaphore_signal(late_sem, inc=1, device_id=(node, peer), device_id_type=MESH)

    for neighbour, flag in zip(neighbours, earlier):

        @pl.when(flag)
        def _(neighbour=neighbour):
            pl.semaphore_signal(node_sem, inc=1, device_id=(neighbour, harm), device_id_type=MESH)

    load_halo.wait()
    for i in range(len(OFFSETS) * slots):
        halo_out_ref[i] = blocks_ref[halo_ref[i, node]]
    empty = block_count + len(OFFSETS) * slots
    blocks_ref[empty] = jnp.zeros(blocks_ref.shape[1:], jnp.bfloat16)
    halo = [
        pltpu.make_async_remote_copy(
            src_ref=halo_out_ref.at[pl.ds(j * slots, slots)],
            dst_ref=halo_in_ref.at[pl.ds(j * slots, slots)],
            send_sem=halo_send_sem.at[j],
            recv_sem=halo_recv_sem.at[j],
            device_id=(neighbour, harm),
            device_id_type=MESH,
        )
        for j, neighbour in enumerate(neighbours)
    ]
    for copy, flag in zip(halo, earlier):
        pl.when(flag)(copy.start)
    for copy in [*for_linear, load_coupling]:
        copy.start()
    for c in range(CHUNKS):
        columns_ref[blocks_of(c, harm)] = blocks_ref[blocks_of(c, harm)]

    @pl.when(proxy)
    def _():
        for c in range(CHUNKS):
            proxy_ref[blocks_of(c, 1)] = blocks_ref[blocks_of(c, 0)]

    for copy in for_nonlinear:
        copy.wait()

    def bytes_of(buffer, blocks, sem):
        part = buffer.at[pl.ds(0, blocks)]
        return pltpu.make_async_copy(part, part, sem)

    def evaluate(row, read, write):
        taken = jnp.concatenate(
            [jnp.concatenate([read(q, p) for q in range(n_harm)], axis=0) for p in range(points)],
            axis=1,
        )
        voltage = jnp.dot(synthesis_ref[...], taken, preferred_element_type=jnp.float32)

        def wide(values):
            return jnp.concatenate([values] * points, axis=1)

        steep = wide(steepness_ref[row] * LOG2_E)
        scale = wide(saturation_ref[row] * LN_2)
        junction = wide(junction_ref[row])
        drive = steep * voltage
        current = scale * (
            jnp.maximum(drive, 0.0) + jnp.log(1.0 + jnp.exp2(-jnp.abs(drive))) * LOG2_E - 1.0
        )
        charge = junction * voltage * lax.rsqrt(1.0 + voltage * voltage)
        both = jnp.concatenate([current.astype(jnp.bfloat16), charge.astype(jnp.bfloat16)], axis=0)
        combined = jnp.dot(analysis_ref[...], both, preferred_element_type=jnp.float32)
        combined = combined.astype(jnp.bfloat16)
        for q in range(n_harm):
            for p in range(points):
                write(
                    q,
                    p,
                    combined[
                        q * spec_rows : (q + 1) * spec_rows,
                        p * block_size : (p + 1) * block_size,
                    ],
                )

    def give(c, owner, given_ref, peer, send_sem):
        return pltpu.make_async_remote_copy(
            src_ref=given_ref.at[blocks_of(c, peer)],
            dst_ref=result_ref.at[blocks_of(c, owner)],
            send_sem=send_sem,
            recv_sem=back_recv_sem.at[c],
            device_id=(node, peer),
            device_id_type=MESH,
        )

    deferring = (node == 0) & (harm > 1)

    def evaluate_chunk(c, owner, taken_ref, given_ref, send_sem):
        for i in range(PIECES[c]):

            def read(q, p):
                return taken_ref[starts[c] + q * PIECES[c] + i, p]

            def write(q, p, values):
                given_ref[starts[c] + q * PIECES[c] + i, p] = values

            evaluate(pl.ds(starts[c] + owner * PIECES[c] + i, 1), read, write)
        order = [(peer, ~(deferring & (peer == 0))) for peer in peers]
        if c >= CHUNKS - 2:
            order = [(1, harm != 1), (0, (harm != 0) & ~deferring)] + [
                (peer, peer > 1) for peer in peers
            ]
        for peer, flag in order:
            pl.when(flag)(give(c, owner, given_ref, peer, send_sem).start)
        result_ref[blocks_of(c, owner)] = given_ref[blocks_of(c, harm)]

    def nonlinear(c):
        with jax.named_scope(f"there_wait_{c}"):
            bytes_of(columns_ref, (n_harm - 1) * PIECES[c], there_recv_sem.at[c]).wait()
        if c == 0:

            @pl.when(with_last)
            def _():
                with jax.named_scope("last_wait"):
                    pl.semaphore_wait(late_sem, 1)

        evaluate_chunk(c, harm, columns_ref, back_ref, back_send_sem)

        @pl.when(proxy)
        def _():
            with jax.named_scope(f"proxy_wait_{c}"):
                bytes_of(proxy_ref, (n_harm - 1) * PIECES[c], proxy_sem.at[c]).wait()
            evaluate_chunk(c, 0, proxy_ref, proxy_back_ref, proxy_sem.at[CHUNKS])

    row_index = lax.broadcasted_iota(jnp.int32, (1, 8, block_size), 1)
    even = row_index % 2 == 0
    tiles = spec_rows // 8
    pulsations = []
    for i in range(tiles):
        harmonic = (harm * spec_rows + i * 8 + row_index) // 2
        value = harmonic.astype(jnp.float32) * (2.0 / rows)
        pulsations.append(jnp.where(even, value, -value))
    pulsation = jnp.concatenate(pulsations * points, axis=0)

    def couple(b, carry):
        gathered = jnp.concatenate(
            [
                blocks_ref[slot_ref[k, b]].reshape(points * spec_rows, block_size)
                for k in range(listed)
            ],
            axis=1,
        )
        matrix = jnp.concatenate([coupling_ref[b, k] for k in range(listed)], axis=1)
        coupled = lax.dot_general(
            gathered, matrix, (((1,), (1,)), ((), ())), preferred_element_type=jnp.float32
        )
        columns = columns_of(b)
        stored = capacitance_ref[pl.ds(b, 1)] * spectrum_ref[:, :, columns].reshape(
            points * spec_rows, block_size
        )
        stored = stored.reshape(points * tiles, 8, block_size)
        swapped = jnp.where(even, pltpu.roll(stored, 7, 1), pltpu.roll(stored, 1, 1))
        linear = (pulsation * swapped).reshape(points, spec_rows, block_size)
        out_ref[:, :, columns] = (
            coupled.reshape(points, spec_rows, block_size) + linear - source_ref[:, :, columns]
        )
        return carry

    with jax.named_scope("node_wait"):
        awaited = count(later)

        @pl.when(awaited > 0)
        def _():
            pl.semaphore_wait(node_sem, awaited)

    for copy, flag in zip(halo, later):
        pl.when(flag)(copy.start)

    def take_halo():
        with jax.named_scope("halo_wait"):
            for j, copy in enumerate(halo):
                opposite = len(OFFSETS) - 1 - j
                pl.when(later[opposite] | earlier[opposite])(copy.wait_recv)
        blocks_ref[pl.ds(block_count, len(OFFSETS) * slots)] = halo_in_ref[...]
        for copy in [*for_linear, load_coupling]:
            copy.wait()

    def couple_part(part, carry):
        first = part * per_part
        for i in range(per_part):
            couple(first + i, 0)
        return carry

    early = jnp.where(proxy, EARLY_PARTS, 0)

    @pl.when(proxy)
    def _():
        take_halo()
        with jax.named_scope("couple_early"):
            lax.fori_loop(0, EARLY_PARTS, couple_part, 0)

    @pl.when(~last)
    def _():
        for c in range(CHUNKS):
            nonlinear(c)

        @pl.when(deferring)
        def _():
            for c in range(CHUNKS):
                give(c, harm, back_ref, 0, back_send_sem).start()

    pl.when(~proxy)(take_halo)
    with jax.named_scope("couple"):
        lax.fori_loop(early, COUPLING_PARTS, couple_part, 0)

    def wait_blocks(flag, buffer, blocks, sem):
        pl.when(flag)(lambda: bytes_of(buffer, blocks, sem).wait())

    plain = ~last & ~proxy
    for c in range(CHUNKS):
        with jax.named_scope(f"back_wait_{c}"):
            wait_blocks(plain, result_ref, (n_harm - 1) * PIECES[c], back_recv_sem.at[c])
            wait_blocks(proxy, result_ref, (n_harm - 2) * PIECES[c], back_recv_sem.at[c])
            wait_blocks(last, result_ref, n_harm * PIECES[c], back_recv_sem.at[c])
        if c == CHUNKS - 1:
            with jax.named_scope("sent"):
                for copy, up, down in zip(halo, later, earlier):
                    pl.when(up | down)(copy.wait_send)
                wait_blocks(plain, blocks_ref, (n_harm - 1) * share, there_send_sem)
                wait_blocks(proxy, blocks_ref, (n_harm - 2) * share, there_send_sem)
                wait_blocks(last, blocks_ref, n_harm * share, there_send_sem)
                wait_blocks(~last, back_ref, (n_harm - 1) * share, back_send_sem)
                wait_blocks(proxy, back_ref, (n_harm - 1) * share, proxy_sem.at[CHUNKS])
        with jax.named_scope(f"add_{c}"):
            for b in range(starts[c], starts[c + 1]):
                at = pl.ds(b * block_size, block_size)
                out_ref[:, :, at] += result_ref[b].astype(jnp.float32)


def solution(mesh):
    n_node, n_harm = mesh.shape["node"], mesh.shape["harm"]

    def local(
        spectrum,
        source,
        coupling,
        capacitance,
        saturation,
        steepness,
        junction,
        halo_list,
        neighbour_slot,
    ):
        spec_rows, points, node_count = spectrum.shape
        block_count, listed, block_size, _ = coupling.shape
        rows = spec_rows * n_harm
        slots = halo_list.shape[2]
        synthesis, analysis = tables(rows)
        halo_count = len(OFFSETS) * slots
        block = (points, spec_rows, block_size)
        held = functools.partial(pltpu.with_memory_space_constraint, memory_space=pltpu.HBM)
        dma = pltpu.SemaphoreType.DMA
        result = pl.pallas_call(
            functools.partial(body, n_node, n_harm),
            name="residual",
            out_shape=pltpu.VMEM((points, spec_rows, node_count), jnp.float32),
            in_specs=[pl.BlockSpec(memory_space=pltpu.HBM)] * 11,
            out_specs=pl.BlockSpec(memory_space=pltpu.VMEM),
            scratch_shapes=[
                pltpu.SMEM((halo_count, n_node), jnp.int32),
                pltpu.SMEM((listed, block_count), jnp.int32),
                *[pltpu.VMEM((block_count, block_size), jnp.float32)] * 4,
                pltpu.VMEM((rows, rows), jnp.bfloat16),
                pltpu.VMEM((rows, 2 * rows), jnp.bfloat16),
                pltpu.VMEM((points, spec_rows, node_count), jnp.float32),
                pltpu.VMEM((points, spec_rows, node_count), jnp.float32),
                pltpu.VMEM(coupling.shape, jnp.bfloat16),
                pltpu.VMEM((block_count + halo_count + 1, *block), jnp.bfloat16),
                pltpu.VMEM((halo_count, *block), jnp.bfloat16),
                pltpu.VMEM((halo_count, *block), jnp.bfloat16),
                *[pltpu.VMEM((block_count, *block), jnp.bfloat16)] * 3,
                dma((9,)),
                dma((CHUNKS,)),
                dma,
                dma((len(OFFSETS),)),
                dma((len(OFFSETS),)),
                dma,
                dma((CHUNKS,)),
                dma,
                dma((CHUNKS,)),
                pltpu.SemaphoreType.REGULAR,
                pltpu.SemaphoreType.REGULAR,
                pltpu.VMEM((block_count, *block), jnp.bfloat16),
                pltpu.VMEM((block_count, *block), jnp.bfloat16),
                dma((CHUNKS + 1,)),
            ],
            compiler_params=pltpu.CompilerParams(
                collective_id=0, has_side_effects=True, vmem_limit_bytes=40 * 2**20
            ),
        )(
            held(halo_list.transpose(1, 2, 0).reshape(halo_count, n_node)),
            held(neighbour_slot.T),
            held(spectrum.transpose(1, 0, 2)),
            held(source.transpose(1, 0, 2)),
            held(coupling),
            held(capacitance.reshape(block_count, block_size)),
            held(saturation.reshape(block_count, block_size)),
            held(steepness.reshape(block_count, block_size)),
            held(junction.reshape(block_count, block_size)),
            held(jnp.asarray(synthesis, jnp.bfloat16)),
            held(jnp.asarray(analysis, jnp.bfloat16)),
        )
        return result.transpose(1, 0, 2)

    return jax.shard_map(
        local,
        mesh=mesh,
        in_specs=(
            P("harm", None, "node"),
            P("harm", None, "node"),
            P("node", None, None, None),
            P("node"),
            P("node"),
            P("node"),
            P("node"),
            P(),
            P("node", None),
        ),
        out_specs=P("harm", None, "node"),
        check_vma=False,
    )
```
